512 devices in a mesh: dp: 128 (over z, y, core), mp: 4 (over x).
Axes of the slice: x: 4, y: 8, z: 8, core: 2. Of those that a mesh axis runs over, the one named last changes fastest.
Arguments:
- tokens: bfloat16 [32768, 4096], P('dp', 'mp'), may hold values from -6 to 6
- router_weight: bfloat16 [4096, 64], P('mp'), may hold values from -1 to 1
- valid_count: int32 [128], P('dp'), may hold values from 64 to 256, as said below
- expert_id: int32 [32768], P('dp'), may hold values from 0 to 63, as said below
- slot_id: int32 [32768], P('dp'), may hold values from 0 to 5
Outputs:
- gates: float32 [32768], P('dp')
- dispatched: bfloat16 [384, 128, 4096], P('dp', None, 'mp')
The draws below stay inside these ranges and needn't reach their ends.
Inputs may be any that keep to these rules, and one draw needn't show every extreme that they name: Group g's live tokens are its first valid_count[g] positions; the last group is full. Within one group no two positions share an expert and a slot. Flat slots expert_id * 6 + slot_id are held 3 in a row by one owner; one group's positions take at most 2 slots of any owner, and in every group some owner has 2 of its slots taken by live tokens.
All inputs are finite; a program needn't handle non-finite values.
Results may differ from the reference program's by a relative error of at most 0.001.
Values may be sent and summed in bfloat16 or wider, within the bound.
A program may use at most 64 MiB of HBM per device.

```python
import jax
import jax.numpy as jnp

D = 4096
E = 64
ITERS = 5
TOK_DEV = 256
CAP = 6
TOKENS = 32768
SEND = 2


def draw_valid_count(key, part):
    groups = TOKENS // TOK_DEV
    lowest = TOK_DEV // 4
    index = jnp.arange(groups, dtype=jnp.int32)
    rising = lowest + (TOK_DEV - lowest) * index // max(groups - 1, 1)
    jitter = jax.random.randint(jax.random.fold_in(key, 11), (groups,), 0, TOK_DEV // 8 + 1)
    counts = jnp.maximum(rising - jitter, lowest)
    return jnp.where(index == groups - 1, TOK_DEV, counts).astype(jnp.int32)


def slot_table(key):
    base_key = jax.random.fold_in(key, 7)
    groups = TOKENS // TOK_DEV
    block_size = E * CAP // groups
    most = SEND
    pool_size = groups * most

    def one_group(group_key):
        owner_keys = jax.random.split(jax.random.fold_in(group_key, 1), groups)

        def owner_pick(owner_key):
            return jax.random.permutation(owner_key, block_size)[:most].astype(jnp.int32)
        picks = jax.vmap(owner_pick)(owner_keys)
        owners = jnp.arange(groups, dtype=jnp.int32)
        flat = (owners[:, None] * block_size + picks).reshape(-1)
        front = jax.random.randint(jax.random.fold_in(group_key, 2), (), 0, groups)
        score = jax.random.permutation(jax.random.fold_in(group_key, 3), pool_size).astype(jnp.int32)
        owner_of = jnp.arange(pool_size, dtype=jnp.int32) // most
        score = jnp.where(owner_of == front, score - pool_size, score)
        order = jnp.argsort(score)
        return flat[order][:TOK_DEV].astype(jnp.int32)

    def group_key_of(number):
        return jax.random.fold_in(base_key, number + 100)
    group_keys = jax.vmap(group_key_of)(jnp.arange(groups, dtype=jnp.int32))
    return jax.vmap(one_group)(group_keys).reshape(-1)


def draw_expert_id(key, part):
    return (slot_table(key) // CAP).astype(jnp.int32)


def draw_slot_id(key, part):
    return (slot_table(key) % CAP).astype(jnp.int32)


def steps_of(stream_key, extent, cuts, least, top_value):
    def one(dim, shards_of):
        draws = jax.random.uniform(jax.random.fold_in(jax.random.fold_in(stream_key, 6), dim), (shards_of,), jnp.float32, least / len(cuts), top_value / len(cuts))
        return jnp.repeat(jnp.exp(draws), extent[dim] // shards_of).reshape((-1,) + (1,) * (len(extent) - dim - 1))

    loudness = one(*cuts[0])
    for cut in cuts[1:]:
        loudness = loudness * one(*cut)
    return loudness


def noise(stream_key, shape, scale, bound, cuts=(), held_as=jnp.bfloat16):
    result = jax.random.normal(stream_key, shape, jnp.float32) * scale
    if len(cuts) > 0:
        result = steps_of(stream_key, shape, cuts, -0.22, 0.18) * result
    return jnp.clip(result, min=-bound, max=bound).astype(held_as)


def setup_inputs(seed: int = 0) -> dict:
    key_of = jax.random.split(jax.random.key(seed), 6)
    tokens = noise(key_of[0], (TOKENS, D), 1.0, 6.0, ((0, 128), (1, 4)))
    router_weight = noise(key_of[1], (D, E), (4.0 * D ** -0.5), 1.0, ((0, 4),))
    valid_count = draw_valid_count(jax.random.fold_in(key_of[5], 71), 0)
    expert_id = draw_expert_id(jax.random.fold_in(key_of[5], 71), 0)
    slot_id = draw_slot_id(jax.random.fold_in(key_of[5], 71), 0)
    return dict(tokens=tokens, router_weight=router_weight, valid_count=valid_count, expert_id=expert_id, slot_id=slot_id)


def reference(tokens, router_weight, valid_count, expert_id, slot_id):
    logits = jnp.dot(tokens, router_weight, preferred_element_type=jnp.float32)
    affinity = jnp.exp(logits)
    groups = valid_count.shape[0]
    indices = jnp.arange(TOKENS, dtype=jnp.int32)
    position = indices % TOK_DEV
    group_of = indices // TOK_DEV
    live = position < valid_count[group_of]
    weight = live.astype(jnp.float32)
    total = jnp.sum(valid_count.astype(jnp.float32))
    col_scale = jnp.ones((E,), jnp.float32)
    row_scale = jnp.ones((TOKENS,), jnp.float32)
    for sweep in range(ITERS):
        row_scale = E / jnp.sum(affinity * col_scale[None, :], axis=1)
        column = jnp.sum(affinity * (weight * row_scale)[:, None], axis=0)
        col_scale = total / column
    chosen = expert_id[:, None] == jnp.arange(E, dtype=jnp.int32)[None, :]
    picked = jnp.sum(jnp.where(chosen, affinity * col_scale[None, :], 0.0), axis=1)
    gates = weight * row_scale * picked
    outside = E * CAP * groups
    target = jnp.where(live, (expert_id * CAP + slot_id) * groups + group_of, outside)
    buffer = jnp.zeros((outside, tokens.shape[1]), jnp.bfloat16).at[target].set(tokens, mode="drop")
    dispatched = buffer.reshape(E * CAP, groups, tokens.shape[1])
    return gates, dispatched
```

```python
import functools

import jax
import jax.numpy as jnp
from jax import lax
from jax.experimental import pallas as pl
from jax.experimental.pallas import tpu as pltpu
from jax.sharding import PartitionSpec as P

E = 64
CAP = 6
ITERS = 5
GROUPS = 128
LINE = 8
XN = 4
ROWS = 256
WIDE = 1024
HELD = 3
META = 128
MESH = pl.DeviceIdType.MESH
NT = (((1,), (1,)), ((), ()))


def f32dot(a, b):
    return jnp.dot(a, b, preferred_element_type=jnp.float32)


def ntdot(a, b):
    return lax.dot_general(a, b, NT, preferred_element_type=jnp.float32)


def split2(x):
    hi = x.astype(jnp.bfloat16)
    lo = (x - hi.astype(jnp.float32)).astype(jnp.bfloat16)
    return hi, lo


def route(
    count_ref, eid_ref, sid_ref, w_ref, tok_hbm,
    gates_ref, land_ref,
    tok_ref, pack_ref, lp_ref, rs_ref, full_ref, gt_ref, gb_ref, mine_ref, ar_ref,
    tok_sem, send_sem, rs_sem, ag_sem, g_sem, ar_sem, d_sem,
):
    dp = lax.axis_index("dp")
    mp = lax.axis_index("mp")
    core = lax.rem(dp, 2)
    y = lax.rem(lax.div(dp, 2), LINE)
    z = lax.div(dp, 2 * LINE)
    mate = dp + 1 - 2 * core

    def x_of(k):
        return lax.rem(mp + k, XN)

    def y_peer(k):
        return z * 16 + lax.rem(y + k, LINE) * 2 + core

    def z_peer(k):
        return lax.rem(z + k, LINE) * 16 + y * 2 + core

    fetch = pltpu.make_async_copy(tok_hbm, tok_ref, tok_sem)
    fetch.start()

    barrier = pltpu.get_barrier_semaphore()
    for k in range(1, XN):
        pl.semaphore_signal(barrier, inc=1, device_id=(dp, x_of(k)), device_id_type=MESH)
        pl.semaphore_signal(barrier, inc=1, device_id=(mate, x_of(k)), device_id_type=MESH)

    @pl.loop(1, GROUPS)
    def _(k):
        pl.semaphore_signal(
            barrier, inc=1, device_id=(lax.rem(dp + k, GROUPS), mp), device_id_type=MESH
        )

    def send(src, dst, ssem, rsem, device):
        pltpu.make_async_remote_copy(
            src_ref=src, dst_ref=dst, send_sem=ssem, recv_sem=rsem,
            device_id=device, device_id_type=MESH,
        ).start()

    def settle(ref, sem):
        pltpu.make_async_copy(ref, ref, sem).wait()

    count = count_ref[0]
    lane = lax.broadcasted_iota(jnp.int32, (128, 128), 1)
    row = lax.broadcasted_iota(jnp.int32, (128, 128), 0)
    low = lane < E
    same = (lane < E) == (row < E)

    target = eid_ref[...] * CAP + sid_ref[...]
    place = lax.broadcasted_iota(jnp.int32, (1, ROWS), 1)
    target = jnp.where(place < count, target, -1)
    slot_row = lax.broadcasted_iota(jnp.int32, (2 * GROUPS, ROWS), 0)
    owner = lax.div(slot_row, 2)
    first = lax.rem(slot_row, 2) == 0
    offset = target - HELD * owner
    at = [jnp.where(offset == s, 1.0, 0.0) for s in range(HELD)]
    used = [jnp.sum(a, axis=1, keepdims=True) for a in at]
    none0 = 1.0 - used[0]
    none01 = none0 * (1.0 - used[1])
    pick0 = at[0] + at[1] * none0 + at[2] * none01
    pick1 = at[1] * (1.0 - none0) + at[2] * (1.0 - none01)
    pick = jnp.where(first, pick0, pick1).astype(jnp.bfloat16)
    code = jnp.broadcast_to(used[0] + 2.0 * used[1] + 4.0 * used[2], (2 * GROUPS, META))

    eid = eid_ref[...].astype(jnp.float32)
    eid_lo = jnp.broadcast_to(eid[:, :128], (128, 128)).T
    eid_hi = jnp.broadcast_to(eid[:, 128:], (128, 128)).T
    chosen = jnp.where(low, eid_lo, eid_hi) == lax.rem(lane, E).astype(jnp.float32)
    live = jnp.where(low, row, row + 128) < count

    fetch.wait()
    la = f32dot(tok_ref[:128, :], w_ref[...])
    lb = f32dot(tok_ref[128:, :], w_ref[...])
    lp_ref[...] = jnp.concatenate([la, lb], axis=1).reshape(XN, 32, 128)

    pl.semaphore_wait(barrier, GROUPS - 1 + 2 * (XN - 1))

    for k in range(1, XN):
        send(lp_ref.at[x_of(k)], rs_ref.at[k - 1], send_sem.at[0], rs_sem, (dp, x_of(k)))

    for j in range(0, WIDE, 256):
        part = f32dot(pick, tok_ref[:, j : j + 256]).astype(jnp.bfloat16)
        pack_ref[:, :, j : j + 256] = part.reshape(GROUPS, 2, 256)
    pack_ref[:, :, WIDE:] = code.astype(jnp.bfloat16).reshape(GROUPS, 2, META)
    land_ref[dp] = pack_ref[dp]

    settle(rs_ref, rs_sem)
    logits = lp_ref[mp] + rs_ref[0] + rs_ref[1] + rs_ref[2]
    full_ref[mp] = logits
    for k in range(1, XN):
        send(full_ref.at[mp], full_ref.at[mp], send_sem.at[1], ag_sem, (dp, x_of(k)))

    qlane = lax.broadcasted_iota(jnp.int32, (32, 128), 1)
    qtok = lax.broadcasted_iota(jnp.int32, (32, 128), 0) + 32 * mp
    qtok = jnp.where(qlane < E, qtok, qtok + 128)
    mixed = lax.rem((dp * ROWS + qtok) * 40503, 65536).astype(jnp.float32)
    dither = 1.0 - mixed * (0.5 / 65536)
    held = jnp.where(qtok < count, jnp.exp(logits) * dither, 0.0).astype(jnp.bfloat16)
    gt_ref[z, y] = held[:16]
    gb_ref[y, z] = held[16:]

    for k in range(1, LINE):
        send(gt_ref.at[z, y], gt_ref.at[z, y], send_sem.at[2], g_sem.at[0], (y_peer(k), mp))
        send(gb_ref.at[y, z], gb_ref.at[y, z], send_sem.at[3], g_sem.at[1], (z_peer(k), mp))
    settle(gt_ref.at[0, pl.ds(0, LINE - 1)], g_sem.at[0])
    for k in range(1, LINE):
        send(gt_ref.at[z], gt_ref.at[z], send_sem.at[4], g_sem.at[2], (z_peer(k), mp))
    settle(gb_ref.at[0, pl.ds(0, LINE - 1)], g_sem.at[1])
    for k in range(1, LINE):
        send(gb_ref.at[y], gb_ref.at[y], send_sem.at[5], g_sem.at[3], (y_peer(k), mp))

    @pl.loop(1, GROUPS)
    def _(k):
        peer = lax.rem(dp + k, GROUPS)
        send(pack_ref.at[peer], land_ref.at[dp], send_sem.at[6], d_sem, (peer, mp))

    settle(gt_ref.at[pl.ds(0, LINE - 1)], g_sem.at[2])
    settle(gb_ref.at[pl.ds(0, LINE - 1)], g_sem.at[3])

    me = mp * 2 + core
    col = jnp.ones((1, 128), jnp.float32)
    before = col
    total = None
    for it in range(ITERS):
        hi, lo = split2(jnp.where(same, jnp.broadcast_to(col, (128, 128)), 0.0))
        acc = jnp.zeros((1, 128), jnp.float32)
        seen = jnp.zeros((1, 128), jnp.float32)
        for ref in (gt_ref, gb_ref):
            for b in range(LINE):
                aff = ref[b].reshape(128, 128)
                rows = ntdot(aff, hi)
                if it > 0:
                    rows = rows + ntdot(aff, lo)
                there = rows > 0.0
                scale = E / jnp.where(there, rows, 1.0)
                acc = acc + jnp.sum(aff.astype(jnp.float32) * scale, axis=0, keepdims=True)
                if it == 0:
                    seen = seen + jnp.sum(jnp.where(there, 1.0, 0.0), axis=0, keepdims=True)
        acc = acc + pltpu.roll(acc, E, 1)
        seen = seen + pltpu.roll(seen, E, 1)
        both = jnp.concatenate([acc, seen], axis=0)
        mine_ref[it] = both
        ar_ref[it, me] = both
        for k in range(XN):
            for other in range(2):
                if k == 0 and other == 0:
                    continue
                device = (mate if other else dp, x_of(k))
                send(mine_ref.at[it], ar_ref.at[it, me], send_sem.at[7], ar_sem.at[it], device)
        settle(ar_ref.at[it, pl.ds(0, 7)], ar_sem.at[it])
        summed = jnp.sum(ar_ref[it], axis=0)
        if it == 0:
            total = summed[1:2]
        before = col
        col = total / summed[0:1]

    settle(full_ref.at[pl.ds(0, XN - 1)], ag_sem)
    aff = jnp.exp(full_ref[...].reshape(128, 128))
    ones = jnp.where(same, 1.0, 0.0).astype(jnp.bfloat16)
    bh, bl = split2(aff * before)
    rows = f32dot(bh, ones) + f32dot(bl, ones)
    gate = jnp.where(chosen & live, aff * col * (E / rows), 0.0)
    srow = lax.broadcasted_iota(jnp.int32, (8, 128), 0)
    slane = lax.broadcasted_iota(jnp.int32, (8, 128), 1)
    side = jnp.where(lax.div(slane, E) == srow, 1.0, 0.0).astype(jnp.bfloat16)
    g1, rest = gate.astype(jnp.bfloat16), None
    rest = gate - g1.astype(jnp.float32)
    g2, g3 = split2(rest)
    out = ntdot(side, g1) + ntdot(side, g2) + ntdot(side, g3)
    gates_ref[...] = out[:2]

    settle(land_ref.at[pl.ds(0, GROUPS - 1)], d_sem)
    settle(rs_ref, send_sem.at[0])
    settle(rs_ref, send_sem.at[1])
    settle(gt_ref.at[0, pl.ds(0, LINE - 1)], send_sem.at[2])
    settle(gt_ref.at[0, pl.ds(0, LINE - 1)], send_sem.at[3])
    settle(gt_ref.at[pl.ds(0, LINE - 1)], send_sem.at[4])
    settle(gt_ref.at[pl.ds(0, LINE - 1)], send_sem.at[5])
    settle(land_ref.at[pl.ds(0, GROUPS - 1)], send_sem.at[6])
    for it in range(ITERS):
        settle(ar_ref.at[it, pl.ds(0, 7)], send_sem.at[7])


def expand(land_ref, gates_ref, out_ref, gout_ref):
    gout_ref[...] = gates_ref[...]
    code = land_ref[:, :, WIDE:].reshape(2 * GROUPS, META).astype(jnp.int32)
    second = lax.rem(lax.broadcasted_iota(jnp.int32, (2 * GROUPS, META), 0), 2)
    bits = [lax.rem(lax.div(code, 2**s), 2) for s in range(HELD)]
    below = [jnp.zeros_like(code), bits[0], bits[0] + bits[1]]
    take = [
        jnp.where((bits[s] == 1) & (below[s] == second), 1.0, 0.0).astype(jnp.bfloat16)
        for s in range(HELD)
    ]
    r = lax.broadcasted_iota(jnp.int32, (GROUPS, 2 * GROUPS), 0)
    c = lax.broadcasted_iota(jnp.int32, (GROUPS, 2 * GROUPS), 1)
    fold = jnp.where(lax.div(c, 2) == r, 1.0, 0.0).astype(jnp.bfloat16)
    for j in range(0, WIDE, 128):
        part = land_ref[:, :, j : j + 128].reshape(2 * GROUPS, 128)
        for s in range(HELD):
            out_ref[s, :, j : j + 128] = f32dot(fold, part * take[s]).astype(jnp.bfloat16)


def local(tokens, router_weight, valid_count, expert_id, slot_id):
    vmem = pl.BlockSpec(memory_space=pltpu.VMEM)
    bf, f32 = jnp.bfloat16, jnp.float32
    gates, land = pl.pallas_call(
        route,
        out_shape=(
            jax.ShapeDtypeStruct((2, 128), f32),
            jax.ShapeDtypeStruct((GROUPS, 2, WIDE + META), bf),
        ),
        in_specs=[
            pl.BlockSpec(memory_space=pltpu.SMEM), vmem, vmem, vmem,
            pl.BlockSpec(memory_space=pl.ANY),
        ],
        out_specs=(vmem, vmem),
        scratch_shapes=[
            pltpu.VMEM((ROWS, WIDE), bf),
            pltpu.VMEM((GROUPS, 2, WIDE + META), bf),
            pltpu.VMEM((XN, 32, 128), f32),
            pltpu.VMEM((XN - 1, 32, 128), f32),
            pltpu.VMEM((XN, 32, 128), f32),
            pltpu.VMEM((LINE, LINE, 16, 128), bf),
            pltpu.VMEM((LINE, LINE, 16, 128), bf),
            pltpu.VMEM((ITERS, 2, 128), f32),
            pltpu.VMEM((ITERS, 8, 2, 128), f32),
            pltpu.SemaphoreType.DMA,
            pltpu.SemaphoreType.DMA((8,)),
            pltpu.SemaphoreType.DMA,
            pltpu.SemaphoreType.DMA,
            pltpu.SemaphoreType.DMA((4,)),
            pltpu.SemaphoreType.DMA((ITERS,)),
            pltpu.SemaphoreType.DMA,
        ],
        compiler_params=pltpu.CompilerParams(collective_id=0, has_side_effects=True),
        name="route",
    )(valid_count, expert_id.reshape(1, ROWS), slot_id.reshape(1, ROWS), router_weight, tokens)
    dispatched, gates = pl.pallas_call(
        expand,
        out_shape=(
            jax.ShapeDtypeStruct((HELD, GROUPS, WIDE), bf),
            jax.ShapeDtypeStruct((2, 128), f32),
        ),
        in_specs=[vmem, vmem],
        out_specs=(vmem, vmem),
        name="expand",
    )(land, gates)
    return gates.reshape(ROWS), dispatched


def solution(mesh):
    return jax.shard_map(
        local,
        mesh=mesh,
        in_specs=(P("dp", "mp"), P("mp", None), P("dp"), P("dp"), P("dp")),
        out_specs=(P("dp"), P("dp", None, "mp")),
        check_vma=False,
    )
```

```python
import functools

import jax
import jax.numpy as jnp
from jax import lax
from jax.experimental import pallas as pl
from jax.experimental.pallas import tpu as pltpu
from jax.sharding import PartitionSpec as P

E = 64
CAP = 6
ITERS = 5
GROUPS = 128
LINE = 8
SPOTS = 64
XN = 4
ROWS = 256
WIDE = 1024
HELD = 3
META = 128
MESH = pl.DeviceIdType.MESH
NT = (((1,), (1,)), ((), ()))


def f32dot(a, b):
    return jnp.dot(a, b, preferred_element_type=jnp.float32)


def ntdot(a, b):
    return lax.dot_general(a, b, NT, preferred_element_type=jnp.float32)


def split2(x):
    hi = x.astype(jnp.bfloat16)
    lo = (x - hi.astype(jnp.float32)).astype(jnp.bfloat16)
    return hi, lo


def route(
    count_hbm, eid_ref, sid_ref, w_ref, tok_hbm,
    gates_ref, out_hbm,
    held_count, tok_ref, pack_ref, comb_ref, land_ref, lp_ref, rs_ref, full_ref, gt_ref, gb_ref, ar_ref, out_ref,
    count_sem, tok_sem, send_sem, rs_sem, ag_sem, g_sem, ar_sem, m_sem, d_sem, out_sem,
):
    dp = lax.axis_index("dp")
    mp = lax.axis_index("mp")
    core = lax.rem(dp, 2)
    spot = lax.div(dp, 2)
    y = lax.rem(spot, LINE)
    z = lax.div(spot, LINE)
    mate = dp + 1 - 2 * core

    def x_of(k):
        return lax.rem(mp + k, XN)

    def y_peer(k):
        return z * 16 + lax.rem(y + k, LINE) * 2 + core

    def z_peer(k):
        return lax.rem(z + k, LINE) * 16 + y * 2 + core

    fetch = pltpu.make_async_copy(tok_hbm, tok_ref, tok_sem)
    fetch.start()
    counted = pltpu.make_async_copy(count_hbm, held_count, count_sem)
    counted.start()

    barrier = pltpu.get_barrier_semaphore()

    def greet(device):
        pl.semaphore_signal(barrier, inc=1, device_id=device, device_id_type=MESH)

    for k in range(1, LINE):
        greet((y_peer(k), mp))
        greet((z_peer(k), mp))
    greet((mate, mp))
    for k in range(1, XN):
        greet((dp, x_of(k)))
        greet((mate, x_of(k)))

    def send(src, dst, ssem, rsem, device):
        pltpu.make_async_remote_copy(
            src_ref=src, dst_ref=dst, send_sem=ssem, recv_sem=rsem,
            device_id=device, device_id_type=MESH,
        ).start()

    def settle(ref, sem):
        pltpu.make_async_copy(ref, ref, sem).wait()

    fetch.wait()
    whole = ntdot(w_ref[...], tok_ref[...])
    la, lb = whole[:, :128].T, whole[:, 128:].T
    lp_ref[...] = jnp.concatenate([la, lb], axis=1).reshape(XN, 32, 128)

    pl.semaphore_wait(barrier, 2 * (LINE - 1) + 1 + 2 * (XN - 1))

    for k in range(1, XN):
        send(lp_ref.at[x_of(k)], rs_ref.at[k - 1], send_sem.at[0], rs_sem, (dp, x_of(k)))

    lane = lax.broadcasted_iota(jnp.int32, (128, 128), 1)
    row = lax.broadcasted_iota(jnp.int32, (128, 128), 0)
    low = lane < E
    same = (lane < E) == (row < E)

    counted.wait()
    count = held_count[0]
    target = eid_ref[...] * CAP + sid_ref[...]
    place = lax.broadcasted_iota(jnp.int32, (1, ROWS), 1)
    target = jnp.where(place < count, target, -1)
    slot_row = lax.broadcasted_iota(jnp.int32, (2 * GROUPS, ROWS), 0)
    owner = lax.div(lax.rem(slot_row, GROUPS), 2) * 2 + lax.div(slot_row, GROUPS)
    first = lax.rem(slot_row, 2) == 0
    offset = target - HELD * owner
    at = [jnp.where(offset == s, 1.0, 0.0) for s in range(HELD)]
    used = [jnp.sum(a, axis=1, keepdims=True) for a in at]
    none0 = 1.0 - used[0]
    none01 = none0 * (1.0 - used[1])
    pick0 = at[0] + at[1] * none0 + at[2] * none01
    pick1 = at[1] * (1.0 - none0) + at[2] * (1.0 - none01)
    pick = jnp.where(first, pick0, pick1).astype(jnp.bfloat16)
    code = jnp.broadcast_to(used[0] + 2.0 * used[1] + 4.0 * used[2], (2 * GROUPS, META))
    for j in range(0, WIDE, 256):
        part = f32dot(pick, tok_ref[:, j : j + 256]).astype(jnp.bfloat16)
        pack_ref[:, :, :, j : j + 256] = part.reshape(2, SPOTS, 2, 256)
    pack_ref[:, :, :, WIDE:] = code.astype(jnp.bfloat16).reshape(2, SPOTS, 2, META)
    send(pack_ref.at[1 - core], comb_ref.at[core], send_sem.at[6], m_sem, (mate, mp))
    comb_ref[core] = pack_ref[core]

    settle(rs_ref, rs_sem)
    logits = lp_ref[mp] + rs_ref[0] + rs_ref[1] + rs_ref[2]
    full_ref[mp] = logits

    qlane = lax.broadcasted_iota(jnp.int32, (32, 128), 1)
    qtok = lax.broadcasted_iota(jnp.int32, (32, 128), 0) + 32 * mp
    qtok = jnp.where(qlane < E, qtok, qtok + 128)
    mixed = lax.rem((dp * ROWS + qtok) * 40503, 65536).astype(jnp.float32)
    dither = 1.0 - mixed * (0.5 / 65536)
    held = jnp.where(qtok < count, jnp.exp(logits) * dither, 0.0).astype(jnp.bfloat16)
    gt_ref[z, y] = held[:16]
    gb_ref[y, z] = held[16:]

    for k in range(1, LINE):
        send(gt_ref.at[z, y], gt_ref.at[z, y], send_sem.at[2], g_sem.at[0], (y_peer(k), mp))
        send(gb_ref.at[y, z], gb_ref.at[y, z], send_sem.at[3], g_sem.at[1], (z_peer(k), mp))
    for k in range(1, XN):
        send(full_ref.at[mp], full_ref.at[mp], send_sem.at[1], ag_sem, (dp, x_of(k)))

    eid = eid_ref[...].astype(jnp.float32)
    eid_lo = jnp.broadcast_to(eid[:, :128], (128, 128)).T
    eid_hi = jnp.broadcast_to(eid[:, 128:], (128, 128)).T
    chosen = jnp.where(low, eid_lo, eid_hi) == lax.rem(lane, E).astype(jnp.float32)
    chosen = chosen & (jnp.where(low, row, row + 128) < count)

    settle(gt_ref.at[0, pl.ds(0, LINE - 1)], g_sem.at[0])
    for k in range(1, LINE):
        send(gt_ref.at[z], gt_ref.at[z], send_sem.at[4], g_sem.at[2], (z_peer(k), mp))
    settle(gb_ref.at[0, pl.ds(0, LINE - 1)], g_sem.at[1])
    for k in range(1, LINE):
        send(gb_ref.at[y], gb_ref.at[y], send_sem.at[5], g_sem.at[3], (y_peer(k), mp))

    settle(comb_ref.at[0], m_sem)
    for s in range(2):
        land_ref[spot, s] = comb_ref[s, spot]
    settle(gt_ref.at[pl.ds(0, LINE - 1)], g_sem.at[2])
    settle(gb_ref.at[pl.ds(0, LINE - 1)], g_sem.at[3])

    @pl.loop(1, SPOTS)
    def _(k):
        peer = lax.rem(spot + k, SPOTS)
        device = (peer * 2 + core, mp)
        send(comb_ref.at[:, peer], land_ref.at[spot], send_sem.at[7], d_sem, device)

    me = mp * 2 + core
    col = jnp.ones((1, 128), jnp.float32)
    before = col
    total = None
    for it in range(ITERS):
        hi, lo = split2(jnp.where(same, jnp.broadcast_to(col, (128, 128)), 0.0))
        acc = jnp.zeros((1, 128), jnp.float32)
        seen = jnp.zeros((1, 128), jnp.float32)
        for ref in (gt_ref, gb_ref):
            for b in range(LINE):
                aff = ref[b].reshape(128, 128)
                rows = ntdot(aff, hi)
                if it > 0:
                    rows = rows + ntdot(aff, lo)
                there = rows > 0.0
                scale = E / jnp.where(there, rows, 1.0)
                acc = acc + jnp.sum(aff.astype(jnp.float32) * scale, axis=0, keepdims=True)
                if it == 0:
                    seen = seen + jnp.sum(jnp.where(there, 1.0, 0.0), axis=0, keepdims=True)
        acc = acc + pltpu.roll(acc, E, 1)
        seen = seen + pltpu.roll(seen, E, 1)
        ar_ref[it, me] = jnp.concatenate([acc, seen], axis=0)
        for k in range(XN):
            for other in range(2):
                if k == 0 and other == 0:
                    continue
                device = (mate if other else dp, x_of(k))
                send(ar_ref.at[it, me], ar_ref.at[it, me], send_sem.at[8], ar_sem.at[it], device)
        if it == ITERS - 1:
            settle(land_ref.at[pl.ds(0, SPOTS - 1)], d_sem)
            expand(land_ref, out_ref)
            put = pltpu.make_async_copy(out_ref, out_hbm, out_sem)
            put.start()
        settle(ar_ref.at[it, pl.ds(0, 7)], ar_sem.at[it])
        summed = jnp.sum(ar_ref[it], axis=0)
        if it == 0:
            total = summed[1:2]
        before = col
        col = total / summed[0:1]

    settle(full_ref.at[pl.ds(0, XN - 1)], ag_sem)
    aff = jnp.exp(full_ref[...].reshape(128, 128))
    ones = jnp.where(same, 1.0, 0.0).astype(jnp.bfloat16)
    bh, bl = split2(aff * before)
    rows = f32dot(bh, ones) + f32dot(bl, ones)
    gate = jnp.where(chosen, aff * col * (E / rows), 0.0)
    srow = lax.broadcasted_iota(jnp.int32, (8, 128), 0)
    slane = lax.broadcasted_iota(jnp.int32, (8, 128), 1)
    side = jnp.where(lax.div(slane, E) == srow, 1.0, 0.0).astype(jnp.bfloat16)
    g1 = gate.astype(jnp.bfloat16)
    g2, g3 = split2(gate - g1.astype(jnp.float32))
    out = ntdot(side, g1) + ntdot(side, g2) + ntdot(side, g3)
    gates_ref[...] = out[:2]

    put.wait()
    settle(rs_ref, send_sem.at[0])
    settle(rs_ref, send_sem.at[1])
    settle(gt_ref.at[0, pl.ds(0, LINE - 1)], send_sem.at[2])
    settle(gt_ref.at[0, pl.ds(0, LINE - 1)], send_sem.at[3])
    settle(gt_ref.at[pl.ds(0, LINE - 1)], send_sem.at[4])
    settle(gt_ref.at[pl.ds(0, LINE - 1)], send_sem.at[5])
    settle(comb_ref.at[0], send_sem.at[6])
    settle(land_ref.at[pl.ds(0, SPOTS - 1)], send_sem.at[7])
    for it in range(ITERS):
        settle(ar_ref.at[it, pl.ds(0, 7)], send_sem.at[8])


def expand(land_ref, out_ref):
    rows = 2 * GROUPS
    code = land_ref[:, :, :, WIDE:].reshape(rows, META).astype(jnp.int32)
    second = lax.rem(lax.broadcasted_iota(jnp.int32, (rows, META), 0), 2)
    bits = [lax.rem(lax.div(code, 2**s), 2) for s in range(HELD)]
    below = [jnp.zeros_like(code), bits[0], bits[0] + bits[1]]
    take = [
        jnp.where((bits[s] == 1) & (below[s] == second), 1.0, 0.0).astype(jnp.bfloat16)
        for s in range(HELD)
    ]
    r = lax.broadcasted_iota(jnp.int32, (GROUPS, rows), 0)
    c = lax.broadcasted_iota(jnp.int32, (GROUPS, rows), 1)
    fold = jnp.where(lax.div(c, 2) == r, 1.0, 0.0).astype(jnp.bfloat16)
    for j in range(0, WIDE, 128):
        part = land_ref[:, :, :, j : j + 128].reshape(rows, 128)
        for s in range(HELD):
            out_ref[s, :, j : j + 128] = f32dot(fold, part * take[s]).astype(jnp.bfloat16)


def local(tokens, router_weight, valid_count, expert_id, slot_id):
    vmem = pl.BlockSpec(memory_space=pltpu.VMEM)
    anywhere = pl.BlockSpec(memory_space=pl.ANY)
    bf, f32 = jnp.bfloat16, jnp.float32
    gates, dispatched = pl.pallas_call(
        route,
        out_shape=(
            jax.ShapeDtypeStruct((2, 128), f32),
            jax.ShapeDtypeStruct((HELD, GROUPS, WIDE), bf),
        ),
        in_specs=[anywhere, vmem, vmem, vmem, anywhere],
        out_specs=(vmem, anywhere),
        scratch_shapes=[
            pltpu.SMEM((1,), jnp.int32),
            pltpu.VMEM((ROWS, WIDE), bf),
            pltpu.VMEM((2, SPOTS, 2, WIDE + META), bf),
            pltpu.VMEM((2, SPOTS, 2, WIDE + META), bf),
            pltpu.VMEM((SPOTS, 2, 2, WIDE + META), bf),
            pltpu.VMEM((XN, 32, 128), f32),
            pltpu.VMEM((XN - 1, 32, 128), f32),
            pltpu.VMEM((XN, 32, 128), f32),
            pltpu.VMEM((LINE, LINE, 16, 128), bf),
            pltpu.VMEM((LINE, LINE, 16, 128), bf),
            pltpu.VMEM((ITERS, 8, 2, 128), f32),
            pltpu.VMEM((HELD, GROUPS, WIDE), bf),
            pltpu.SemaphoreType.DMA,
            pltpu.SemaphoreType.DMA,
            pltpu.SemaphoreType.DMA((9,)),
            pltpu.SemaphoreType.DMA,
            pltpu.SemaphoreType.DMA,
            pltpu.SemaphoreType.DMA((4,)),
            pltpu.SemaphoreType.DMA((ITERS,)),
            pltpu.SemaphoreType.DMA,
            pltpu.SemaphoreType.DMA,
            pltpu.SemaphoreType.DMA,
        ],
        compiler_params=pltpu.CompilerParams(collective_id=0, has_side_effects=True),
        name="route",
    )(
        valid_count, expert_id.reshape(1, ROWS), slot_id.reshape(1, ROWS),
        router_weight.T, tokens,
    )
    return gates.reshape(ROWS), dispatched


def solution(mesh):
    return jax.shard_map(
        local,
        mesh=mesh,
        in_specs=(P("dp", "mp"), P("mp", None), P("dp"), P("dp"), P("dp")),
        out_specs=(P("dp"), P("dp", None, "mp")),
        check_vma=False,
    )
```

```python
import functools

import jax
import jax.numpy as jnp
from jax import lax
from jax.experimental import pallas as pl
from jax.experimental.pallas import tpu as pltpu
from jax.sharding import PartitionSpec as P

E = 64
CAP = 6
ITERS = 5
GROUPS = 128
LINE = 8
SPOTS = 64
XN = 4
ROWS = 256
WIDE = 1024
HELD = 3
META = 128
MESH = pl.DeviceIdType.MESH
NT = (((1,), (1,)), ((), ()))


def f32dot(a, b):
    return jnp.dot(a, b, preferred_element_type=jnp.float32)


def ntdot(a, b):
    return lax.dot_general(a, b, NT, preferred_element_type=jnp.float32)


def split2(x):
    hi = x.astype(jnp.bfloat16)
    lo = (x - hi.astype(jnp.float32)).astype(jnp.bfloat16)
    return hi, lo


def route(
    count_ref, eid_hbm, sid_hbm, w_hbm, tok_hbm,
    out_ref, full_ref, mask_ref, scale_ref,
    eid_ref, sid_ref, w_ref, tok_ref,
    pack_ref, comb_ref, land_ref, lp_ref, rs_ref, gt_ref, gb_ref, ar_ref,
    in_sem, send_sem, rs_sem, ag_sem, g_sem, ar_sem, m_sem, d_sem,
):
    dp = lax.axis_index("dp")
    mp = lax.axis_index("mp")
    core = lax.rem(dp, 2)
    spot = lax.div(dp, 2)
    y = lax.rem(spot, LINE)
    z = lax.div(spot, LINE)
    mate = dp + 1 - 2 * core

    def x_of(k):
        return lax.rem(mp + k, XN)

    def y_peer(k):
        return z * 16 + lax.rem(y + k, LINE) * 2 + core

    def z_peer(k):
        return lax.rem(z + k, LINE) * 16 + y * 2 + core

    fetches = [
        pltpu.make_async_copy(src, dst, in_sem.at[i])
        for i, (src, dst) in enumerate((
            (w_hbm, w_ref), (tok_hbm, tok_ref), (eid_hbm, eid_ref), (sid_hbm, sid_ref),
        ))
    ]
    for fetch in fetches:
        fetch.start()

    barrier = pltpu.get_barrier_semaphore()

    def greet(device):
        pl.semaphore_signal(barrier, inc=1, device_id=device, device_id_type=MESH)

    for k in range(1, LINE):
        greet((y_peer(k), mp))
        greet((z_peer(k), mp))
    greet((mate, mp))
    for k in range(1, XN):
        greet((dp, x_of(k)))
        greet((mate, x_of(k)))

    def send(src, dst, ssem, rsem, device):
        pltpu.make_async_remote_copy(
            src_ref=src, dst_ref=dst, send_sem=ssem, recv_sem=rsem,
            device_id=device, device_id_type=MESH,
        ).start()

    def settle(ref, sem):
        pltpu.make_async_copy(ref, ref, sem).wait()

    fetches[0].wait()
    fetches[1].wait()
    whole = ntdot(w_ref[...], tok_ref[...])
    la, lb = whole[:, :128].T, whole[:, 128:].T
    lp_ref[...] = jnp.concatenate([la, lb], axis=1).reshape(XN, 32, 128)

    pl.semaphore_wait(barrier, 2 * (LINE - 1) + 1 + 2 * (XN - 1))

    for k in range(1, XN):
        send(lp_ref.at[x_of(k)], rs_ref.at[k - 1], send_sem.at[0], rs_sem, (dp, x_of(k)))

    lane = lax.broadcasted_iota(jnp.int32, (128, 128), 1)
    row = lax.broadcasted_iota(jnp.int32, (128, 128), 0)
    low = lane < E
    same = (lane < E) == (row < E)

    for fetch in fetches[2:]:
        fetch.wait()
    count = count_ref[0]
    target = eid_ref[...] * CAP + sid_ref[...]
    place = lax.broadcasted_iota(jnp.int32, (1, ROWS), 1)
    target = jnp.where(place < count, target, -1)
    slot_row = lax.broadcasted_iota(jnp.int32, (2 * GROUPS, ROWS), 0)
    owner = lax.div(lax.rem(slot_row, GROUPS), 2) * 2 + lax.div(slot_row, GROUPS)
    first = lax.rem(slot_row, 2) == 0
    offset = target - HELD * owner
    at = [jnp.where(offset == s, 1.0, 0.0) for s in range(HELD)]
    used = [jnp.sum(a, axis=1, keepdims=True) for a in at]
    none0 = 1.0 - used[0]
    none01 = none0 * (1.0 - used[1])
    pick0 = at[0] + at[1] * none0 + at[2] * none01
    pick1 = at[1] * (1.0 - none0) + at[2] * (1.0 - none01)
    pick = jnp.where(first, pick0, pick1).astype(jnp.bfloat16)
    code = jnp.broadcast_to(used[0] + 2.0 * used[1] + 4.0 * used[2], (2 * GROUPS, META))
    for j in range(0, WIDE, 256):
        part = f32dot(pick, tok_ref[:, j : j + 256]).astype(jnp.bfloat16)
        pack_ref[:, :, :, j : j + 256] = part.reshape(2, SPOTS, 2, 256)
    pack_ref[:, :, :, WIDE:] = code.astype(jnp.bfloat16).reshape(2, SPOTS, 2, META)
    send(pack_ref.at[1 - core], comb_ref.at[core], send_sem.at[6], m_sem, (mate, mp))
    comb_ref[core] = pack_ref[core]

    settle(rs_ref, rs_sem)
    logits = lp_ref[mp] + rs_ref[0] + rs_ref[1] + rs_ref[2]
    full_ref[mp] = logits

    qlane = lax.broadcasted_iota(jnp.int32, (32, 128), 1)
    qtok = lax.broadcasted_iota(jnp.int32, (32, 128), 0) + 32 * mp
    qtok = jnp.where(qlane < E, qtok, qtok + 128)
    mixed = lax.rem((dp * ROWS + qtok) * 40503, 65536).astype(jnp.float32)
    dither = 1.0 - mixed * (0.5 / 65536)
    held = jnp.where(qtok < count, jnp.exp(logits) * dither, 0.0).astype(jnp.bfloat16)
    gt_ref[z, y] = held[:16]
    gb_ref[y, z] = held[16:]

    for k in range(1, LINE):
        send(gt_ref.at[z, y], gt_ref.at[z, y], send_sem.at[2], g_sem.at[0], (y_peer(k), mp))
        send(gb_ref.at[y, z], gb_ref.at[y, z], send_sem.at[3], g_sem.at[1], (z_peer(k), mp))
    for k in range(1, XN):
        send(full_ref.at[mp], full_ref.at[mp], send_sem.at[1], ag_sem, (dp, x_of(k)))

    eid = eid_ref[...].astype(jnp.float32)
    eid_lo = jnp.broadcast_to(eid[:, :128], (128, 128)).T
    eid_hi = jnp.broadcast_to(eid[:, 128:], (128, 128)).T
    chosen = jnp.where(low, eid_lo, eid_hi) == lax.rem(lane, E).astype(jnp.float32)
    chosen = chosen & (jnp.where(low, row, row + 128) < count)
    mask_ref[...] = jnp.where(chosen, 1.0, 0.0)

    settle(gt_ref.at[0, pl.ds(0, LINE - 1)], g_sem.at[0])
    for k in range(1, LINE):
        send(gt_ref.at[z], gt_ref.at[z], send_sem.at[4], g_sem.at[2], (z_peer(k), mp))
    settle(gb_ref.at[0, pl.ds(0, LINE - 1)], g_sem.at[1])
    for k in range(1, LINE):
        send(gb_ref.at[y], gb_ref.at[y], send_sem.at[5], g_sem.at[3], (y_peer(k), mp))

    settle(comb_ref.at[0], m_sem)
    for s in range(2):
        land_ref[spot, s] = comb_ref[s, spot]
    settle(gt_ref.at[pl.ds(0, LINE - 1)], g_sem.at[2])
    settle(gb_ref.at[pl.ds(0, LINE - 1)], g_sem.at[3])

    me = mp * 2 + core
    col = jnp.ones((1, 128), jnp.float32)
    before = col
    total = None
    for it in range(ITERS):
        hi, lo = split2(jnp.where(same, jnp.broadcast_to(col, (128, 128)), 0.0))
        acc = jnp.zeros((1, 128), jnp.float32)
        seen = jnp.zeros((1, 128), jnp.float32)
        for ref in (gt_ref, gb_ref):
            for b in range(LINE):
                aff = ref[b].reshape(128, 128)
                rows = ntdot(aff, hi)
                if it > 0:
                    rows = rows + ntdot(aff, lo)
                there = rows > 0.0
                scale = E / jnp.where(there, rows, 1.0)
                acc = acc + jnp.sum(aff.astype(jnp.float32) * scale, axis=0, keepdims=True)
                if it == 0:
                    seen = seen + jnp.sum(jnp.where(there, 1.0, 0.0), axis=0, keepdims=True)
        acc = acc + pltpu.roll(acc, E, 1)
        seen = seen + pltpu.roll(seen, E, 1)
        ar_ref[it, me] = jnp.concatenate([acc, seen], axis=0)
        for k in range(XN):
            for other in range(2):
                if k == 0 and other == 0:
                    continue
                device = (mate if other else dp, x_of(k))
                send(ar_ref.at[it, me], ar_ref.at[it, me], send_sem.at[8], ar_sem.at[it], device)
        if it == 0:
            @pl.loop(1, SPOTS)
            def _(k):
                peer = lax.rem(spot + k, SPOTS)
                device = (peer * 2 + core, mp)
                send(comb_ref.at[:, peer], land_ref.at[spot], send_sem.at[7], d_sem, device)

        if it == ITERS - 1:
            settle(land_ref.at[pl.ds(0, SPOTS - 1)], d_sem)
            expand(land_ref, out_ref)
        settle(ar_ref.at[it, pl.ds(0, 7)], ar_sem.at[it])
        summed = jnp.sum(ar_ref[it], axis=0)
        if it == 0:
            total = summed[1:2]
        before = col
        col = total / summed[0:1]

    scale_ref[...] = jnp.concatenate([before, col], axis=0)
    settle(full_ref.at[pl.ds(0, XN - 1)], ag_sem)

    settle(rs_ref, send_sem.at[0])
    settle(rs_ref, send_sem.at[1])
    settle(gt_ref.at[0, pl.ds(0, LINE - 1)], send_sem.at[2])
    settle(gt_ref.at[0, pl.ds(0, LINE - 1)], send_sem.at[3])
    settle(gt_ref.at[pl.ds(0, LINE - 1)], send_sem.at[4])
    settle(gt_ref.at[pl.ds(0, LINE - 1)], send_sem.at[5])
    settle(comb_ref.at[0], send_sem.at[6])
    settle(land_ref.at[pl.ds(0, SPOTS - 1)], send_sem.at[7])
    for it in range(ITERS):
        settle(ar_ref.at[it, pl.ds(0, 7)], send_sem.at[8])


def expand(land_ref, out_ref):
    rows = 2 * GROUPS
    code = land_ref[:, :, :, WIDE:].reshape(rows, META).astype(jnp.int32)
    second = lax.rem(lax.broadcasted_iota(jnp.int32, (rows, META), 0), 2)
    bits = [lax.rem(lax.div(code, 2**s), 2) for s in range(HELD)]
    below = [jnp.zeros_like(code), bits[0], bits[0] + bits[1]]
    take = [
        jnp.where((bits[s] == 1) & (below[s] == second), 1.0, 0.0).astype(jnp.bfloat16)
        for s in range(HELD)
    ]
    r = lax.broadcasted_iota(jnp.int32, (GROUPS, rows), 0)
    c = lax.broadcasted_iota(jnp.int32, (GROUPS, rows), 1)
    fold = jnp.where(lax.div(c, 2) == r, 1.0, 0.0).astype(jnp.bfloat16)
    for j in range(0, WIDE, 128):
        part = land_ref[:, :, :, j : j + 128].reshape(rows, 128)
        for s in range(HELD):
            out_ref[s, :, j : j + 128] = f32dot(fold, part * take[s]).astype(jnp.bfloat16)


def finish(disp_ref, full_ref, mask_ref, scale_ref, out_hbm, gates_hbm, gates_ref, sem):
    put = pltpu.make_async_copy(disp_ref, out_hbm, sem.at[0])
    put.start()
    lane = lax.broadcasted_iota(jnp.int32, (128, 128), 1)
    row = lax.broadcasted_iota(jnp.int32, (128, 128), 0)
    aff = jnp.exp(full_ref[...].reshape(128, 128))
    ones = jnp.where((lane < E) == (row < E), 1.0, 0.0).astype(jnp.bfloat16)
    bh, bl = split2(aff * scale_ref[0:1])
    rows = f32dot(bh, ones) + f32dot(bl, ones)
    gate = jnp.where(mask_ref[...] > 0.0, aff * scale_ref[1:2] * (E / rows), 0.0)
    srow = lax.broadcasted_iota(jnp.int32, (8, 128), 0)
    slane = lax.broadcasted_iota(jnp.int32, (8, 128), 1)
    side = jnp.where(lax.div(slane, E) == srow, 1.0, 0.0).astype(jnp.bfloat16)
    g1 = gate.astype(jnp.bfloat16)
    g2, g3 = split2(gate - g1.astype(jnp.float32))
    out = ntdot(side, g1) + ntdot(side, g2) + ntdot(side, g3)
    gates_ref[...] = out[:2]
    gput = pltpu.make_async_copy(gates_ref, gates_hbm, sem.at[1])
    gput.start()
    put.wait()
    gput.wait()


def local(tokens, router_weight, valid_count, expert_id, slot_id):
    vmem = pl.BlockSpec(memory_space=pltpu.VMEM)
    hbm = pl.BlockSpec(memory_space=pltpu.HBM)
    bf, f32 = jnp.bfloat16, jnp.float32
    dma = pltpu.SemaphoreType.DMA
    parts = pl.pallas_call(
        route,
        out_shape=(
            jax.ShapeDtypeStruct((HELD, GROUPS, WIDE), bf),
            jax.ShapeDtypeStruct((XN, 32, 128), f32),
            jax.ShapeDtypeStruct((128, 128), f32),
            jax.ShapeDtypeStruct((2, 128), f32),
        ),
        in_specs=[pl.BlockSpec(memory_space=pltpu.SMEM), *[hbm] * 4],
        out_specs=(vmem,) * 4,
        scratch_shapes=[
            pltpu.VMEM((1, ROWS), jnp.int32),
            pltpu.VMEM((1, ROWS), jnp.int32),
            pltpu.VMEM((E, WIDE), bf),
            pltpu.VMEM((ROWS, WIDE), bf),
            pltpu.VMEM((2, SPOTS, 2, WIDE + META), bf),
            pltpu.VMEM((2, SPOTS, 2, WIDE + META), bf),
            pltpu.VMEM((SPOTS, 2, 2, WIDE + META), bf),
            pltpu.VMEM((XN, 32, 128), f32),
            pltpu.VMEM((XN - 1, 32, 128), f32),
            pltpu.VMEM((LINE, LINE, 16, 128), bf),
            pltpu.VMEM((LINE, LINE, 16, 128), bf),
            pltpu.VMEM((ITERS, 8, 2, 128), f32),
            dma((4,)), dma((9,)), dma, dma, dma((4,)), dma((ITERS,)), dma, dma,
        ],
        compiler_params=pltpu.CompilerParams(
            collective_id=0, has_side_effects=True, vmem_limit_bytes=24 * 2**20
        ),
        name="route",
    )(valid_count, *(
        pltpu.with_memory_space_constraint(x, pltpu.HBM)
        for x in (
            expert_id.reshape(1, ROWS), slot_id.reshape(1, ROWS),
            router_weight.T, tokens,
        )
    ))
    dispatched, gates = pl.pallas_call(
        finish,
        out_shape=(
            jax.ShapeDtypeStruct((HELD, GROUPS, WIDE), bf),
            jax.ShapeDtypeStruct((2, 128), f32),
        ),
        in_specs=[vmem] * 4,
        out_specs=(hbm, hbm),
        scratch_shapes=[pltpu.VMEM((2, 128), f32), dma((2,))],
        compiler_params=pltpu.CompilerParams(vmem_limit_bytes=16 * 2**20),
        name="finish",
    )(*parts)
    return gates.reshape(ROWS), dispatched


def solution(mesh):
    return jax.shard_map(
        local,
        mesh=mesh,
        in_specs=(P("dp", "mp"), P("mp", None), P("dp"), P("dp"), P("dp")),
        out_specs=(P("dp"), P("dp", None, "mp")),
        check_vma=False,
    )
```

```python
import functools

import jax
import jax.numpy as jnp
from jax import lax
from jax.experimental import pallas as pl
from jax.experimental.pallas import tpu as pltpu
from jax.sharding import PartitionSpec as P

E = 64
CAP = 6
ITERS = 5
GROUPS = 128
LINE = 8
SPOTS = 64
XN = 4
ROWS = 256
WIDE = 1024
HELD = 3
FAR = (4, 3, 5, 2, 6, 1, 7)
TINY = 0.9e-37
META = 128
MESH = pl.DeviceIdType.MESH
NT = (((1,), (1,)), ((), ()))


def f32dot(a, b):
    return jnp.dot(a, b, preferred_element_type=jnp.float32)


def ntdot(a, b):
    return lax.dot_general(a, b, NT, preferred_element_type=jnp.float32)


def split2(x):
    hi = x.astype(jnp.bfloat16)
    lo = (x - hi.astype(jnp.float32)).astype(jnp.bfloat16)
    return hi, lo


def spread(tile):
    return jnp.concatenate(
        [jnp.broadcast_to(tile[:, k : k + 1], (8, 128)) for k in range(8)], axis=0
    )


def route(
    count_ref, eid_hbm, sid_hbm, w_hbm, tok_hbm,
    out_ref, full_ref, mask_ref, before_ref, last_ref,
    eid_ref, sid_ref, w_ref, tok_ref,
    pack_ref, comb_ref, land_ref, lp_ref, rs_ref, gt_ref, gb_ref, xsum_ref, ar_ref, ysum_ref, zsum_ref, aff_ref,
    in_sem, send_sem, rs_sem, ag_sem, g_sem, ar_sem, m_sem, d_sem, c_sem,
):
    dp = lax.axis_index("dp")
    mp = lax.axis_index("mp")
    core = lax.rem(dp, 2)
    spot = lax.div(dp, 2)
    y = lax.rem(spot, LINE)
    z = lax.div(spot, LINE)
    mate = dp + 1 - 2 * core

    def x_of(k):
        return lax.rem(mp + k, XN)

    def y_peer(k):
        return z * 16 + lax.rem(y + k, LINE) * 2 + core

    def z_peer(k):
        return lax.rem(z + k, LINE) * 16 + y * 2 + core

    fetches = [
        pltpu.make_async_copy(src, dst, in_sem.at[i])
        for i, (src, dst) in enumerate((
            (w_hbm, w_ref), (tok_hbm, tok_ref), (eid_hbm, eid_ref), (sid_hbm, sid_ref),
        ))
    ]
    for fetch in fetches:
        fetch.start()

    barrier = pltpu.get_barrier_semaphore()

    def greet(device):
        pl.semaphore_signal(barrier, inc=1, device_id=device, device_id_type=MESH)

    for k in range(1, LINE):
        greet((y_peer(k), mp))
        greet((z_peer(k), mp))
    greet((mate, mp))
    for k in range(1, XN):
        greet((dp, x_of(k)))
        greet((mate, x_of(k)))

    def send(src, dst, ssem, rsem, device):
        pltpu.make_async_remote_copy(
            src_ref=src, dst_ref=dst, send_sem=ssem, recv_sem=rsem,
            device_id=device, device_id_type=MESH,
        ).start()

    def settle(ref, sem):
        pltpu.make_async_copy(ref, ref, sem).wait()

    fetches[0].wait()
    fetches[1].wait()
    whole = ntdot(w_ref[...], tok_ref[...])
    la, lb = whole[:, :128].T, whole[:, 128:].T
    lp_ref[...] = jnp.concatenate([la, lb], axis=1).reshape(XN, 32, 128)

    pl.semaphore_wait(barrier, 2 * (LINE - 1) + 1 + 2 * (XN - 1))

    for k in (2, 1, 3):
        send(lp_ref.at[x_of(k)], rs_ref.at[k - 1], send_sem.at[0], rs_sem, (dp, x_of(k)))

    lane = lax.broadcasted_iota(jnp.int32, (128, 128), 1)
    row = lax.broadcasted_iota(jnp.int32, (128, 128), 0)
    low = lane < E
    same = (lane < E) == (row < E)

    for fetch in fetches[2:]:
        fetch.wait()
    count = count_ref[0]
    target = eid_ref[...] * CAP + sid_ref[...]
    place = lax.broadcasted_iota(jnp.int32, (1, ROWS), 1)
    target = jnp.where(place < count, target, -1)
    slot_row = lax.broadcasted_iota(jnp.int32, (2 * GROUPS, ROWS), 0)
    owner = lax.div(lax.rem(slot_row, GROUPS), 2) * 2 + lax.div(slot_row, GROUPS)
    first = lax.rem(slot_row, 2) == 0
    offset = target - HELD * owner
    at = [jnp.where(offset == s, 1.0, 0.0) for s in range(HELD)]
    used = [jnp.sum(a, axis=1, keepdims=True) for a in at]
    none0 = 1.0 - used[0]
    none01 = none0 * (1.0 - used[1])
    pick0 = at[0] + at[1] * none0 + at[2] * none01
    pick1 = at[1] * (1.0 - none0) + at[2] * (1.0 - none01)
    pick = jnp.where(first, pick0, pick1).astype(jnp.bfloat16)
    code = jnp.broadcast_to(used[0] + 2.0 * used[1] + 4.0 * used[2], (2 * GROUPS, META))
    for j in range(0, WIDE, 256):
        part = f32dot(pick, tok_ref[:, j : j + 256]).astype(jnp.bfloat16)
        pack_ref[:, :, :, j : j + 256] = part.reshape(2, SPOTS, 2, 256)
    pack_ref[:, :, :, WIDE:] = code.astype(jnp.bfloat16).reshape(2, SPOTS, 2, META)
    send(pack_ref.at[1 - core], comb_ref.at[core], send_sem.at[6], m_sem, (mate, mp))
    comb_ref[core] = pack_ref[core]

    settle(rs_ref, rs_sem)
    logits = lp_ref[mp] + rs_ref[0] + rs_ref[1] + rs_ref[2]
    full_ref[mp] = logits

    qlane = lax.broadcasted_iota(jnp.int32, (32, 128), 1)
    qtok = lax.broadcasted_iota(jnp.int32, (32, 128), 0) + 32 * mp
    qtok = jnp.where(qlane < E, qtok, qtok + 128)
    mixed = lax.rem((dp * ROWS + qtok) * 40503, 65536).astype(jnp.float32)
    dither = 1.0 - mixed * (0.5 / 65536)
    fresh = jnp.where(qtok < count, jnp.exp(logits) * dither, 0.0)
    held = fresh.astype(jnp.bfloat16)
    gt_ref[z, y] = held[:16]
    gb_ref[y, z] = held[16:]

    for k in FAR:
        send(gt_ref.at[z, y], gt_ref.at[z, y], send_sem.at[2], g_sem.at[0], (y_peer(k), mp))
        send(gb_ref.at[y, z], gb_ref.at[y, z], send_sem.at[3], g_sem.at[1], (z_peer(k), mp))

    ones = jnp.where(same, 1.0, 0.0).astype(jnp.bfloat16)
    fh, fl = split2(fresh)
    rows = f32dot(jnp.concatenate([fh, fl], axis=1), jnp.concatenate([ones, ones], axis=0))
    there = rows > 0.0
    acc = jnp.sum(fresh / jnp.where(there, rows, 1.0), axis=0, keepdims=True)
    seen = jnp.sum(jnp.where(there, 1.0, 0.0), axis=0, keepdims=True)
    both = jnp.concatenate([acc, seen], axis=0)
    ysum_ref[y] = both + pltpu.roll(both, E, 1)
    for k in FAR:
        send(ysum_ref.at[y], ysum_ref.at[y], send_sem.at[9], c_sem.at[0], (y_peer(k), mp))
    for k in (2, 1, 3):
        send(full_ref.at[mp], full_ref.at[mp], send_sem.at[1], ag_sem, (dp, x_of(k)))

    eid = eid_ref[...].astype(jnp.float32)
    eid_lo = jnp.broadcast_to(eid[:, :128], (128, 128)).T
    eid_hi = jnp.broadcast_to(eid[:, 128:], (128, 128)).T
    chosen = jnp.where(low, eid_lo, eid_hi) == lax.rem(lane, E).astype(jnp.float32)
    chosen = chosen & (jnp.where(low, row, row + 128) < count)
    mask_ref[...] = jnp.where(chosen, 1.0, 0.0)

    settle(gb_ref.at[0, pl.ds(0, LINE - 1)], g_sem.at[1])
    for k in FAR:
        send(gb_ref.at[y], gb_ref.at[y], send_sem.at[5], g_sem.at[3], (y_peer(k), mp))
    settle(ysum_ref.at[pl.ds(0, LINE - 1)], c_sem.at[0])
    zsum_ref[z] = jnp.sum(ysum_ref[...], axis=0)
    for k in FAR:
        send(zsum_ref.at[z], zsum_ref.at[z], send_sem.at[9], c_sem.at[1], (z_peer(k), mp))
    settle(gt_ref.at[0, pl.ds(0, LINE - 1)], g_sem.at[0])
    for k in FAR:
        send(gt_ref.at[z], gt_ref.at[z], send_sem.at[4], g_sem.at[2], (z_peer(k), mp))

    settle(comb_ref.at[0], m_sem)
    for s in range(2):
        land_ref[spot, s] = comb_ref[s, spot]
    me = mp * 2 + core

    def share(slots, value, rsem):
        slots[me] = value
        for k in (2, 1, 3, 0):
            for other in (1, 0):
                if k == 0 and other == 0:
                    continue
                device = (mate if other else dp, x_of(k))
                send(slots.at[me], slots.at[me], send_sem.at[8], rsem, device)

    settle(zsum_ref.at[pl.ds(0, LINE - 1)], c_sem.at[1])
    share(xsum_ref, jnp.sum(zsum_ref[...], axis=0), c_sem.at[2])

    def dispatch(t):
        def step(i):
            return 4 + lax.div(i + 1, 2) * (1 - 2 * lax.rem(i, 2))

        pz = lax.rem(z + step(lax.div(t, LINE)), LINE)
        py = lax.rem(y + step(lax.rem(t, LINE)), LINE)
        peer = pz * LINE + py
        device = (peer * 2 + core, mp)
        send(comb_ref.at[:, peer], land_ref.at[spot], send_sem.at[7], d_sem, device)

    pl.loop(0, SPOTS - 1)(dispatch)

    settle(xsum_ref.at[pl.ds(0, 7)], c_sem.at[2])
    summed = jnp.sum(xsum_ref[...], axis=0)
    total = summed[1:2] * (1.0 / E)
    col = jnp.broadcast_to(total / summed[0:1], (128, 128)).T[:E]

    settle(gb_ref.at[pl.ds(0, LINE - 1)], g_sem.at[3])
    for b in range(LINE):
        aff_ref[LINE + b] = gb_ref[b].reshape(128, 128).astype(jnp.float32).T
    settle(gt_ref.at[pl.ds(0, LINE - 1)], g_sem.at[2])
    for b in range(LINE):
        aff_ref[b] = gt_ref[b].reshape(128, 128).astype(jnp.float32).T

    tile_lane = lax.broadcasted_iota(jnp.int32, (8, 128), 1)
    for it in range(ITERS - 1):
        acc = jnp.zeros((E, 128), jnp.float32)
        for b in range(2 * LINE):
            for half in range(2):
                aff = aff_ref[b, half * E : half * E + E]
                rows = jnp.sum(aff * col, axis=0, keepdims=True)
                acc = acc + aff * (1.0 / jnp.maximum(rows, TINY))
        acc = jnp.sum(acc, axis=1, keepdims=True)
        tile = jnp.ones((8, 128), jnp.float32)
        for k in range(8):
            tile = jnp.where(tile_lane == k, acc[8 * k : 8 * k + 8], tile)
        share(ar_ref.at[it], tile, ar_sem.at[it])
        if it == ITERS - 2:
            before_ref[...] = jnp.concatenate([col, col], axis=0).T[0:1]
            settle(land_ref.at[pl.ds(0, SPOTS - 1)], d_sem)
            expand(land_ref, out_ref)
        settle(ar_ref.at[it, pl.ds(0, 7)], ar_sem.at[it])
        tile = total / jnp.sum(ar_ref[it], axis=0)
        if it < ITERS - 2:
            col = spread(tile)
        else:
            last_ref[...] = tile

    settle(full_ref.at[pl.ds(0, XN - 1)], ag_sem)

    settle(rs_ref, send_sem.at[0])
    settle(rs_ref, send_sem.at[1])
    settle(gt_ref.at[0, pl.ds(0, LINE - 1)], send_sem.at[2])
    settle(gt_ref.at[0, pl.ds(0, LINE - 1)], send_sem.at[3])
    settle(gt_ref.at[pl.ds(0, LINE - 1)], send_sem.at[4])
    settle(gt_ref.at[pl.ds(0, LINE - 1)], send_sem.at[5])
    settle(comb_ref.at[0], send_sem.at[6])
    settle(land_ref.at[pl.ds(0, SPOTS - 1)], send_sem.at[7])
    for _ in range(2):
        settle(ysum_ref.at[pl.ds(0, LINE - 1)], send_sem.at[9])
    settle(xsum_ref.at[pl.ds(0, 7)], send_sem.at[8])
    for it in range(ITERS - 1):
        settle(ar_ref.at[it, pl.ds(0, 7)], send_sem.at[8])


def expand(land_ref, out_ref):
    rows = 2 * GROUPS
    code = land_ref[:, :, :, WIDE:].reshape(rows, META).astype(jnp.int32)
    second = lax.rem(lax.broadcasted_iota(jnp.int32, (rows, META), 0), 2)
    bits = [lax.rem(lax.div(code, 2**s), 2) for s in range(HELD)]
    below = [jnp.zeros_like(code), bits[0], bits[0] + bits[1]]
    take = [
        jnp.where((bits[s] == 1) & (below[s] == second), 1.0, 0.0).astype(jnp.bfloat16)
        for s in range(HELD)
    ]
    r = lax.broadcasted_iota(jnp.int32, (GROUPS, rows), 0)
    c = lax.broadcasted_iota(jnp.int32, (GROUPS, rows), 1)
    fold = jnp.where(lax.div(c, 2) == r, 1.0, 0.0).astype(jnp.bfloat16)
    for j in range(0, WIDE, 128):
        part = land_ref[:, :, :, j : j + 128].reshape(rows, 128)
        for s in range(HELD):
            out_ref[s, :, j : j + 128] = f32dot(fold, part * take[s]).astype(jnp.bfloat16)


def finish(disp_ref, full_ref, mask_ref, before_ref, last_ref, out_hbm, gates_hbm, gates_ref, sem):
    put = pltpu.make_async_copy(disp_ref, out_hbm, sem.at[0])
    put.start()
    lane = lax.broadcasted_iota(jnp.int32, (128, 128), 1)
    row = lax.broadcasted_iota(jnp.int32, (128, 128), 0)
    aff = jnp.exp(full_ref[...].reshape(128, 128))
    ones = jnp.where((lane < E) == (row < E), 1.0, 0.0).astype(jnp.bfloat16)
    bh, bl = split2(aff * before_ref[...])
    rows = f32dot(bh, ones) + f32dot(bl, ones)
    last = spread(last_ref[...])
    last = jnp.concatenate([last, last], axis=0).T[0:1]
    gate = jnp.where(mask_ref[...] > 0.0, aff * last * (E / rows), 0.0)
    srow = lax.broadcasted_iota(jnp.int32, (8, 128), 0)
    slane = lax.broadcasted_iota(jnp.int32, (8, 128), 1)
    side = jnp.where(lax.div(slane, E) == srow, 1.0, 0.0).astype(jnp.bfloat16)
    g1 = gate.astype(jnp.bfloat16)
    g2, g3 = split2(gate - g1.astype(jnp.float32))
    out = ntdot(side, g1) + ntdot(side, g2) + ntdot(side, g3)
    gates_ref[...] = out[:2]
    gput = pltpu.make_async_copy(gates_ref, gates_hbm, sem.at[1])
    gput.start()
    put.wait()
    gput.wait()


def local(tokens, router_weight, valid_count, expert_id, slot_id):
    vmem = pl.BlockSpec(memory_space=pltpu.VMEM)
    hbm = pl.BlockSpec(memory_space=pltpu.HBM)
    bf, f32 = jnp.bfloat16, jnp.float32
    dma = pltpu.SemaphoreType.DMA
    parts = pl.pallas_call(
        route,
        out_shape=(
            jax.ShapeDtypeStruct((HELD, GROUPS, WIDE), bf),
            jax.ShapeDtypeStruct((XN, 32, 128), f32),
            jax.ShapeDtypeStruct((128, 128), f32),
            jax.ShapeDtypeStruct((1, 128), f32),
            jax.ShapeDtypeStruct((8, 128), f32),
        ),
        in_specs=[pl.BlockSpec(memory_space=pltpu.SMEM), *[hbm] * 4],
        out_specs=(vmem,) * 5,
        scratch_shapes=[
            pltpu.VMEM((1, ROWS), jnp.int32),
            pltpu.VMEM((1, ROWS), jnp.int32),
            pltpu.VMEM((E, WIDE), bf),
            pltpu.VMEM((ROWS, WIDE), bf),
            pltpu.VMEM((2, SPOTS, 2, WIDE + META), bf),
            pltpu.VMEM((2, SPOTS, 2, WIDE + META), bf),
            pltpu.VMEM((SPOTS, 2, 2, WIDE + META), bf),
            pltpu.VMEM((XN, 32, 128), f32),
            pltpu.VMEM((XN - 1, 32, 128), f32),
            pltpu.VMEM((LINE, LINE, 16, 128), bf),
            pltpu.VMEM((LINE, LINE, 16, 128), bf),
            pltpu.VMEM((8, 2, 128), f32),
            pltpu.VMEM((ITERS - 1, 8, 8, 128), f32),
            pltpu.VMEM((LINE, 2, 128), f32),
            pltpu.VMEM((LINE, 2, 128), f32),
            pltpu.VMEM((2 * LINE, 128, 128), f32),
            dma((4,)), dma((10,)), dma, dma, dma((4,)), dma((ITERS - 1,)), dma, dma, dma((3,)),
        ],
        compiler_params=pltpu.CompilerParams(
            collective_id=0, has_side_effects=True, vmem_limit_bytes=24 * 2**20
        ),
        name="route",
    )(valid_count, *(
        pltpu.with_memory_space_constraint(x, pltpu.HBM)
        for x in (
            expert_id.reshape(1, ROWS), slot_id.reshape(1, ROWS),
            router_weight.T, tokens,
        )
    ))
    dispatched, gates = pl.pallas_call(
        finish,
        out_shape=(
            jax.ShapeDtypeStruct((HELD, GROUPS, WIDE), bf),
            jax.ShapeDtypeStruct((2, 128), f32),
        ),
        in_specs=[vmem] * 5,
        out_specs=(hbm, hbm),
        scratch_shapes=[pltpu.VMEM((2, 128), f32), dma((2,))],
        compiler_params=pltpu.CompilerParams(vmem_limit_bytes=16 * 2**20),
        name="finish",
    )(*parts)
    return gates.reshape(ROWS), dispatched


def solution(mesh):
    return jax.shard_map(
        local,
        mesh=mesh,
        in_specs=(P("dp", "mp"), P("mp", None), P("dp"), P("dp"), P("dp")),
        out_specs=(P("dp"), P("dp", None, "mp")),
        check_vma=False,
    )
```

```python
import functools

import jax
import jax.numpy as jnp
from jax import lax
from jax.experimental import pallas as pl
from jax.experimental.pallas import tpu as pltpu
from jax.sharding import PartitionSpec as P

E = 64
CAP = 6
ITERS = 5
GROUPS = 128
LINE = 8
SPOTS = 64
XN = 4
ROWS = 256
WIDE = 1024
HELD = 3
FAR = (4, 3, 5, 2, 6, 1, 7)
TINY = 0.9e-37
AHEAD = 20
META = 128
MESH = pl.DeviceIdType.MESH
NT = (((1,), (1,)), ((), ()))


def f32dot(a, b):
    return jnp.dot(a, b, preferred_element_type=jnp.float32)


def ntdot(a, b):
    return lax.dot_general(a, b, NT, preferred_element_type=jnp.float32)


def split2(x):
    hi = x.astype(jnp.bfloat16)
    lo = (x - hi.astype(jnp.float32)).astype(jnp.bfloat16)
    return hi, lo


def spread(tile):
    return jnp.concatenate(
        [jnp.broadcast_to(tile[:, k : k + 1], (8, 128)) for k in range(8)], axis=0
    )


def route(
    count_ref, eid_hbm, sid_hbm, w_hbm, tok_hbm,
    out_ref, full_ref, mask_ref, before_ref, last_ref,
    eid_ref, sid_ref, w_ref, tok_ref,
    pack_ref, comb_ref, land_ref, lp_ref, rs_ref, gt_ref, gb_ref, xsum_ref, ar_ref, ysum_ref, zsum_ref, aff_ref,
    in_sem, send_sem, rs_sem, ag_sem, g_sem, ar_sem, m_sem, d_sem, c_sem, known_sem,
):
    dp = lax.axis_index("dp")
    mp = lax.axis_index("mp")
    core = lax.rem(dp, 2)
    spot = lax.div(dp, 2)
    y = lax.rem(spot, LINE)
    z = lax.div(spot, LINE)
    mate = dp + 1 - 2 * core

    def x_of(k):
        return lax.rem(mp + k, XN)

    def y_peer(k):
        return z * 16 + lax.rem(y + k, LINE) * 2 + core

    def z_peer(k):
        return lax.rem(z + k, LINE) * 16 + y * 2 + core

    fetches = [
        pltpu.make_async_copy(src, dst, in_sem.at[i])
        for i, (src, dst) in enumerate((
            (w_hbm, w_ref), (tok_hbm, tok_ref), (eid_hbm, eid_ref), (sid_hbm, sid_ref),
        ))
    ]
    for fetch in fetches:
        fetch.start()

    barrier = pltpu.get_barrier_semaphore()

    def greet(device):
        pl.semaphore_signal(barrier, inc=1, device_id=device, device_id_type=MESH)

    for k in range(1, LINE):
        greet((y_peer(k), mp))
        greet((z_peer(k), mp))
    greet((mate, mp))
    for k in range(1, XN):
        greet((dp, x_of(k)))
        greet((mate, x_of(k)))

    def send(src, dst, ssem, rsem, device):
        pltpu.make_async_remote_copy(
            src_ref=src, dst_ref=dst, send_sem=ssem, recv_sem=rsem,
            device_id=device, device_id_type=MESH,
        ).start()

    def settle(ref, sem):
        pltpu.make_async_copy(ref, ref, sem).wait()

    fetches[0].wait()
    fetches[1].wait()
    whole = ntdot(w_ref[...], tok_ref[...])
    la, lb = whole[:, :128].T, whole[:, 128:].T
    lp_ref[...] = jnp.concatenate([la, lb], axis=1).reshape(XN, 32, 128)

    pl.semaphore_wait(barrier, 2 * (LINE - 1) + 1 + 2 * (XN - 1))

    for k in (2, 1, 3):
        send(lp_ref.at[x_of(k)], rs_ref.at[k - 1], send_sem.at[0], rs_sem, (dp, x_of(k)))
    for k in FAR:
        pl.semaphore_signal(
            known_sem, inc=1, device_id=(z_peer(k), mp), device_id_type=MESH
        )

    lane = lax.broadcasted_iota(jnp.int32, (128, 128), 1)
    row = lax.broadcasted_iota(jnp.int32, (128, 128), 0)
    low = lane < E
    same = (lane < E) == (row < E)

    for fetch in fetches[2:]:
        fetch.wait()
    count = count_ref[0]
    target = eid_ref[...] * CAP + sid_ref[...]
    place = lax.broadcasted_iota(jnp.int32, (1, ROWS), 1)
    target = jnp.where(place < count, target, -1)
    slot_row = lax.broadcasted_iota(jnp.int32, (2 * GROUPS, ROWS), 0)
    owner = lax.div(lax.rem(slot_row, GROUPS), 2) * 2 + lax.div(slot_row, GROUPS)
    first = lax.rem(slot_row, 2) == 0
    offset = target - HELD * owner
    at = [jnp.where(offset == s, 1.0, 0.0) for s in range(HELD)]
    used = [jnp.sum(a, axis=1, keepdims=True) for a in at]
    none0 = 1.0 - used[0]
    none01 = none0 * (1.0 - used[1])
    pick0 = at[0] + at[1] * none0 + at[2] * none01
    pick1 = at[1] * (1.0 - none0) + at[2] * (1.0 - none01)
    pick = jnp.where(first, pick0, pick1).astype(jnp.bfloat16)
    code = jnp.broadcast_to(used[0] + 2.0 * used[1] + 4.0 * used[2], (2 * GROUPS, META))
    for j in range(0, WIDE, 256):
        part = f32dot(pick, tok_ref[:, j : j + 256]).astype(jnp.bfloat16)
        pack_ref[:, :, :, j : j + 256] = part.reshape(2, SPOTS, 2, 256)
    pack_ref[:, :, :, WIDE:] = code.astype(jnp.bfloat16).reshape(2, SPOTS, 2, META)
    send(pack_ref.at[1 - core], comb_ref.at[core], send_sem.at[6], m_sem, (mate, mp))
    comb_ref[core] = pack_ref[core]

    settle(rs_ref, rs_sem)
    logits = lp_ref[mp] + rs_ref[0] + rs_ref[1] + rs_ref[2]
    full_ref[mp] = logits

    qlane = lax.broadcasted_iota(jnp.int32, (32, 128), 1)
    qtok = lax.broadcasted_iota(jnp.int32, (32, 128), 0) + 32 * mp
    qtok = jnp.where(qlane < E, qtok, qtok + 128)
    mixed = lax.rem((dp * ROWS + qtok) * 40503, 65536).astype(jnp.float32)
    dither = 1.0 - mixed * (0.5 / 65536)
    fresh = jnp.where(qtok < count, jnp.exp(logits) * dither, 0.0)
    held = fresh.astype(jnp.bfloat16)
    gt_ref[z, y] = held[:16]
    gb_ref[y, z] = held[16:]

    for k in FAR:
        send(gt_ref.at[z, y], gt_ref.at[z, y], send_sem.at[2], g_sem.at[0], (y_peer(k), mp))
        send(gb_ref.at[y, z], gb_ref.at[y, z], send_sem.at[3], g_sem.at[1], (z_peer(k), mp))

    ones = jnp.where(same, 1.0, 0.0).astype(jnp.bfloat16)
    fh, fl = split2(fresh)
    rows = f32dot(jnp.concatenate([fh, fl], axis=1), jnp.concatenate([ones, ones], axis=0))
    there = rows > 0.0
    acc = jnp.sum(fresh / jnp.where(there, rows, 1.0), axis=0, keepdims=True)
    seen = jnp.sum(jnp.where(there, 1.0, 0.0), axis=0, keepdims=True)
    both = jnp.concatenate([acc, seen], axis=0)
    ysum_ref[y] = both + pltpu.roll(both, E, 1)
    for k in FAR:
        send(ysum_ref.at[y], ysum_ref.at[y], send_sem.at[9], c_sem.at[0], (y_peer(k), mp))
    for k in (2, 1, 3):
        send(full_ref.at[mp], full_ref.at[mp], send_sem.at[1], ag_sem, (dp, x_of(k)))

    def dispatch(t):
        pz = lax.rem(z + lax.div(t, LINE) + lax.rem(t, LINE), LINE)
        py = lax.rem(y + t, LINE)
        peer = pz * LINE + py
        device = (peer * 2 + core, mp)
        send(comb_ref.at[:, peer], land_ref.at[spot], send_sem.at[7], d_sem, device)

    settle(comb_ref.at[0], m_sem)
    pl.semaphore_wait(known_sem, LINE - 1)
    pl.loop(1, 1 + AHEAD)(dispatch)

    eid = eid_ref[...].astype(jnp.float32)
    eid_lo = jnp.broadcast_to(eid[:, :128], (128, 128)).T
    eid_hi = jnp.broadcast_to(eid[:, 128:], (128, 128)).T
    chosen = jnp.where(low, eid_lo, eid_hi) == lax.rem(lane, E).astype(jnp.float32)
    chosen = chosen & (jnp.where(low, row, row + 128) < count)
    mask_ref[...] = jnp.where(chosen, 1.0, 0.0)

    settle(gb_ref.at[0, pl.ds(0, LINE - 1)], g_sem.at[1])
    for k in FAR:
        send(gb_ref.at[y], gb_ref.at[y], send_sem.at[5], g_sem.at[3], (y_peer(k), mp))
    settle(ysum_ref.at[pl.ds(0, LINE - 1)], c_sem.at[0])
    zsum_ref[z] = jnp.sum(ysum_ref[...], axis=0)
    for k in FAR:
        send(zsum_ref.at[z], zsum_ref.at[z], send_sem.at[9], c_sem.at[1], (z_peer(k), mp))
    settle(gt_ref.at[0, pl.ds(0, LINE - 1)], g_sem.at[0])
    for k in FAR:
        send(gt_ref.at[z], gt_ref.at[z], send_sem.at[4], g_sem.at[2], (z_peer(k), mp))

    for s in range(2):
        land_ref[spot, s] = comb_ref[s, spot]
    me = mp * 2 + core

    def share(slots, value, rsem):
        slots[me] = value
        for k in (2, 1, 3, 0):
            for other in (1, 0):
                if k == 0 and other == 0:
                    continue
                device = (mate if other else dp, x_of(k))
                send(slots.at[me], slots.at[me], send_sem.at[8], rsem, device)

    settle(zsum_ref.at[pl.ds(0, LINE - 1)], c_sem.at[1])
    share(xsum_ref, jnp.sum(zsum_ref[...], axis=0), c_sem.at[2])

    settle(xsum_ref.at[pl.ds(0, 7)], c_sem.at[2])
    summed = jnp.sum(xsum_ref[...], axis=0)
    total = summed[1:2] * (1.0 / E)
    col = jnp.broadcast_to(total / summed[0:1], (128, 128)).T[:E]

    settle(gb_ref.at[pl.ds(0, LINE - 1)], g_sem.at[3])
    for b in range(LINE):
        aff_ref[LINE + b] = gb_ref[b].reshape(128, 128).astype(jnp.float32).T
    settle(gt_ref.at[pl.ds(0, LINE - 1)], g_sem.at[2])
    for b in range(LINE):
        aff_ref[b] = gt_ref[b].reshape(128, 128).astype(jnp.float32).T

    tile_lane = lax.broadcasted_iota(jnp.int32, (8, 128), 1)
    for it in range(ITERS - 1):
        acc = jnp.zeros((E, 128), jnp.float32)
        for b in range(2 * LINE):
            for half in range(2):
                aff = aff_ref[b, half * E : half * E + E]
                rows = jnp.sum(aff * col, axis=0, keepdims=True)
                acc = acc + aff * (1.0 / jnp.maximum(rows, TINY))
        acc = jnp.sum(acc, axis=1, keepdims=True)
        tile = jnp.ones((8, 128), jnp.float32)
        for k in range(8):
            tile = jnp.where(tile_lane == k, acc[8 * k : 8 * k + 8], tile)
        share(ar_ref.at[it], tile, ar_sem.at[it])
        if it == 0:
            pl.loop(1 + AHEAD, SPOTS)(dispatch)
        if it == ITERS - 2:
            before_ref[...] = jnp.concatenate([col, col], axis=0).T[0:1]
            settle(land_ref.at[pl.ds(0, SPOTS - 1)], d_sem)
            expand(land_ref, out_ref)
        settle(ar_ref.at[it, pl.ds(0, 7)], ar_sem.at[it])
        tile = total / jnp.sum(ar_ref[it], axis=0)
        if it < ITERS - 2:
            col = spread(tile)
        else:
            last_ref[...] = tile

    settle(full_ref.at[pl.ds(0, XN - 1)], ag_sem)

    settle(rs_ref, send_sem.at[0])
    settle(rs_ref, send_sem.at[1])
    settle(gt_ref.at[0, pl.ds(0, LINE - 1)], send_sem.at[2])
    settle(gt_ref.at[0, pl.ds(0, LINE - 1)], send_sem.at[3])
    settle(gt_ref.at[pl.ds(0, LINE - 1)], send_sem.at[4])
    settle(gt_ref.at[pl.ds(0, LINE - 1)], send_sem.at[5])
    settle(comb_ref.at[0], send_sem.at[6])
    settle(land_ref.at[pl.ds(0, SPOTS - 1)], send_sem.at[7])
    for _ in range(2):
        settle(ysum_ref.at[pl.ds(0, LINE - 1)], send_sem.at[9])
    settle(xsum_ref.at[pl.ds(0, 7)], send_sem.at[8])
    for it in range(ITERS - 1):
        settle(ar_ref.at[it, pl.ds(0, 7)], send_sem.at[8])


def expand(land_ref, out_ref):
    rows = 2 * GROUPS
    code = land_ref[:, :, :, WIDE:].reshape(rows, META).astype(jnp.int32)
    second = lax.rem(lax.broadcasted_iota(jnp.int32, (rows, META), 0), 2)
    bits = [lax.rem(lax.div(code, 2**s), 2) for s in range(HELD)]
    below = [jnp.zeros_like(code), bits[0], bits[0] + bits[1]]
    take = [
        jnp.where((bits[s] == 1) & (below[s] == second), 1.0, 0.0).astype(jnp.bfloat16)
        for s in range(HELD)
    ]
    r = lax.broadcasted_iota(jnp.int32, (GROUPS, rows), 0)
    c = lax.broadcasted_iota(jnp.int32, (GROUPS, rows), 1)
    fold = jnp.where(lax.div(c, 2) == r, 1.0, 0.0).astype(jnp.bfloat16)
    for j in range(0, WIDE, 128):
        part = land_ref[:, :, :, j : j + 128].reshape(rows, 128)
        for s in range(HELD):
            out_ref[s, :, j : j + 128] = f32dot(fold, part * take[s]).astype(jnp.bfloat16)


def finish(disp_ref, full_ref, mask_ref, before_ref, last_ref, out_hbm, gates_hbm, gates_ref, sem):
    put = pltpu.make_async_copy(disp_ref, out_hbm, sem.at[0])
    put.start()
    lane = lax.broadcasted_iota(jnp.int32, (128, 128), 1)
    row = lax.broadcasted_iota(jnp.int32, (128, 128), 0)
    aff = jnp.exp(full_ref[...].reshape(128, 128))
    ones = jnp.where((lane < E) == (row < E), 1.0, 0.0).astype(jnp.bfloat16)
    bh, bl = split2(aff * before_ref[...])
    rows = f32dot(bh, ones) + f32dot(bl, ones)
    last = spread(last_ref[...])
    last = jnp.concatenate([last, last], axis=0).T[0:1]
    gate = jnp.where(mask_ref[...] > 0.0, aff * last * (E / rows), 0.0)
    srow = lax.broadcasted_iota(jnp.int32, (8, 128), 0)
    slane = lax.broadcasted_iota(jnp.int32, (8, 128), 1)
    side = jnp.where(lax.div(slane, E) == srow, 1.0, 0.0).astype(jnp.bfloat16)
    g1 = gate.astype(jnp.bfloat16)
    g2, g3 = split2(gate - g1.astype(jnp.float32))
    out = ntdot(side, g1) + ntdot(side, g2) + ntdot(side, g3)
    gates_ref[...] = out[:2]
    gput = pltpu.make_async_copy(gates_ref, gates_hbm, sem.at[1])
    gput.start()
    put.wait()
    gput.wait()


def local(tokens, router_weight, valid_count, expert_id, slot_id):
    vmem = pl.BlockSpec(memory_space=pltpu.VMEM)
    hbm = pl.BlockSpec(memory_space=pltpu.HBM)
    bf, f32 = jnp.bfloat16, jnp.float32
    dma = pltpu.SemaphoreType.DMA
    parts = pl.pallas_call(
        route,
        out_shape=(
            jax.ShapeDtypeStruct((HELD, GROUPS, WIDE), bf),
            jax.ShapeDtypeStruct((XN, 32, 128), f32),
            jax.ShapeDtypeStruct((128, 128), f32),
            jax.ShapeDtypeStruct((1, 128), f32),
            jax.ShapeDtypeStruct((8, 128), f32),
        ),
        in_specs=[pl.BlockSpec(memory_space=pltpu.SMEM), *[hbm] * 4],
        out_specs=(vmem,) * 5,
        scratch_shapes=[
            pltpu.VMEM((1, ROWS), jnp.int32),
            pltpu.VMEM((1, ROWS), jnp.int32),
            pltpu.VMEM((E, WIDE), bf),
            pltpu.VMEM((ROWS, WIDE), bf),
            pltpu.VMEM((2, SPOTS, 2, WIDE + META), bf),
            pltpu.VMEM((2, SPOTS, 2, WIDE + META), bf),
            pltpu.VMEM((SPOTS, 2, 2, WIDE + META), bf),
            pltpu.VMEM((XN, 32, 128), f32),
            pltpu.VMEM((XN - 1, 32, 128), f32),
            pltpu.VMEM((LINE, LINE, 16, 128), bf),
            pltpu.VMEM((LINE, LINE, 16, 128), bf),
            pltpu.VMEM((8, 2, 128), f32),
            pltpu.VMEM((ITERS - 1, 8, 8, 128), f32),
            pltpu.VMEM((LINE, 2, 128), f32),
            pltpu.VMEM((LINE, 2, 128), f32),
            pltpu.VMEM((2 * LINE, 128, 128), f32),
            dma((4,)), dma((10,)), dma, dma, dma((4,)), dma((ITERS - 1,)), dma, dma, dma((3,)),
            pltpu.SemaphoreType.REGULAR,
        ],
        compiler_params=pltpu.CompilerParams(
            collective_id=0, has_side_effects=True, vmem_limit_bytes=24 * 2**20
        ),
        name="route",
    )(valid_count, *(
        pltpu.with_memory_space_constraint(x, pltpu.HBM)
        for x in (
            expert_id.reshape(1, ROWS), slot_id.reshape(1, ROWS),
            router_weight.T, tokens,
        )
    ))
    dispatched, gates = pl.pallas_call(
        finish,
        out_shape=(
            jax.ShapeDtypeStruct((HELD, GROUPS, WIDE), bf),
            jax.ShapeDtypeStruct((2, 128), f32),
        ),
        in_specs=[vmem] * 5,
        out_specs=(hbm, hbm),
        scratch_shapes=[pltpu.VMEM((2, 128), f32), dma((2,))],
        compiler_params=pltpu.CompilerParams(vmem_limit_bytes=16 * 2**20),
        name="finish",
    )(*parts)
    return gates.reshape(ROWS), dispatched


def solution(mesh):
    return jax.shard_map(
        local,
        mesh=mesh,
        in_specs=(P("dp", "mp"), P("mp", None), P("dp"), P("dp"), P("dp")),
        out_specs=(P("dp"), P("dp", None, "mp")),
        check_vma=False,
    )
```

```python
import functools

import jax
import jax.numpy as jnp
from jax import lax
from jax.experimental import pallas as pl
from jax.experimental.pallas import tpu as pltpu
from jax.sharding import PartitionSpec as P

E = 64
CAP = 6
ITERS = 5
GROUPS = 128
LINE = 8
SPOTS = 64
XN = 4
ROWS = 256
WIDE = 1024
HELD = 3
FAR = (4, 3, 5, 2, 6, 1, 7)
TINY = 0.9e-37
AHEAD = 20


def steps_away(t):
    return min(t[0], LINE - t[0]) + min(t[1], LINE - t[1])


ORDER = sorted(
    ((a, b) for a in range(LINE) for b in range(LINE) if a + b > 0),
    key=lambda t: (-steps_away(t), (t[0] + t[1]) % LINE, t),
)
ORDER = ORDER[-AHEAD:] + ORDER[:-AHEAD]
META = 128
MESH = pl.DeviceIdType.MESH
NT = (((1,), (1,)), ((), ()))


def f32dot(a, b):
    return jnp.dot(a, b, preferred_element_type=jnp.float32)


def ntdot(a, b):
    return lax.dot_general(a, b, NT, preferred_element_type=jnp.float32)


def split2(x):
    hi = x.astype(jnp.bfloat16)
    lo = (x - hi.astype(jnp.float32)).astype(jnp.bfloat16)
    return hi, lo


def spread(tile):
    return jnp.concatenate(
        [jnp.broadcast_to(tile[:, k : k + 1], (8, 128)) for k in range(8)], axis=0
    )


def route(
    count_ref, eid_hbm, sid_hbm, w_hbm, tok_hbm,
    out_ref, full_ref, mask_ref, before_ref, last_ref,
    eid_ref, sid_ref, w_ref, tok_ref,
    pack_ref, comb_ref, land_ref, lp_ref, rs_ref, gt_ref, gb_ref, xsum_ref, ar_ref, ysum_ref, zsum_ref, aff_ref,
    in_sem, send_sem, rs_sem, ag_sem, g_sem, ar_sem, m_sem, d_sem, c_sem, known_sem,
):
    dp = lax.axis_index("dp")
    mp = lax.axis_index("mp")
    core = lax.rem(dp, 2)
    spot = lax.div(dp, 2)
    y = lax.rem(spot, LINE)
    z = lax.div(spot, LINE)
    mate = dp + 1 - 2 * core

    def x_of(k):
        return lax.rem(mp + k, XN)

    def y_peer(k):
        return z * 16 + lax.rem(y + k, LINE) * 2 + core

    def z_peer(k):
        return lax.rem(z + k, LINE) * 16 + y * 2 + core

    fetches = [
        pltpu.make_async_copy(src, dst, in_sem.at[i])
        for i, (src, dst) in enumerate((
            (w_hbm, w_ref), (tok_hbm, tok_ref), (eid_hbm, eid_ref), (sid_hbm, sid_ref),
        ))
    ]
    for fetch in fetches:
        fetch.start()

    barrier = pltpu.get_barrier_semaphore()

    def greet(device):
        pl.semaphore_signal(barrier, inc=1, device_id=device, device_id_type=MESH)

    for k in range(1, LINE):
        greet((y_peer(k), mp))
        greet((z_peer(k), mp))
    greet((mate, mp))
    for k in range(1, XN):
        greet((dp, x_of(k)))
        greet((mate, x_of(k)))

    def send(src, dst, ssem, rsem, device):
        pltpu.make_async_remote_copy(
            src_ref=src, dst_ref=dst, send_sem=ssem, recv_sem=rsem,
            device_id=device, device_id_type=MESH,
        ).start()

    def settle(ref, sem):
        pltpu.make_async_copy(ref, ref, sem).wait()

    fetches[0].wait()
    fetches[1].wait()
    whole = ntdot(w_ref[...], tok_ref[...])
    la, lb = whole[:, :128].T, whole[:, 128:].T
    lp_ref[...] = jnp.concatenate([la, lb], axis=1).reshape(XN, 32, 128)

    pl.semaphore_wait(barrier, 2 * (LINE - 1) + 1 + 2 * (XN - 1))

    for k in (2, 1, 3):
        send(lp_ref.at[x_of(k)], rs_ref.at[k - 1], send_sem.at[0], rs_sem, (dp, x_of(k)))
    for k in FAR:
        pl.semaphore_signal(
            known_sem, inc=1, device_id=(z_peer(k), mp), device_id_type=MESH
        )

    lane = lax.broadcasted_iota(jnp.int32, (128, 128), 1)
    row = lax.broadcasted_iota(jnp.int32, (128, 128), 0)
    low = lane < E
    same = (lane < E) == (row < E)

    for fetch in fetches[2:]:
        fetch.wait()
    count = count_ref[0]
    target = eid_ref[...] * CAP + sid_ref[...]
    place = lax.broadcasted_iota(jnp.int32, (1, ROWS), 1)
    target = jnp.where(place < count, target, -1)
    slot_row = lax.broadcasted_iota(jnp.int32, (2 * GROUPS, ROWS), 0)
    owner = lax.div(lax.rem(slot_row, GROUPS), 2) * 2 + lax.div(slot_row, GROUPS)
    first = lax.rem(slot_row, 2) == 0
    offset = target - HELD * owner
    at = [jnp.where(offset == s, 1.0, 0.0) for s in range(HELD)]
    used = [jnp.sum(a, axis=1, keepdims=True) for a in at]
    none0 = 1.0 - used[0]
    none01 = none0 * (1.0 - used[1])
    pick0 = at[0] + at[1] * none0 + at[2] * none01
    pick1 = at[1] * (1.0 - none0) + at[2] * (1.0 - none01)
    pick = jnp.where(first, pick0, pick1).astype(jnp.bfloat16)
    code = jnp.broadcast_to(used[0] + 2.0 * used[1] + 4.0 * used[2], (2 * GROUPS, META))
    for j in range(0, WIDE, 256):
        part = f32dot(pick, tok_ref[:, j : j + 256]).astype(jnp.bfloat16)
        pack_ref[:, :, :, j : j + 256] = part.reshape(2, SPOTS, 2, 256)
    pack_ref[:, :, :, WIDE:] = code.astype(jnp.bfloat16).reshape(2, SPOTS, 2, META)
    send(pack_ref.at[1 - core], comb_ref.at[core], send_sem.at[6], m_sem, (mate, mp))
    comb_ref[core] = pack_ref[core]

    settle(rs_ref, rs_sem)
    logits = lp_ref[mp] + rs_ref[0] + rs_ref[1] + rs_ref[2]
    full_ref[mp] = logits

    qlane = lax.broadcasted_iota(jnp.int32, (32, 128), 1)
    qtok = lax.broadcasted_iota(jnp.int32, (32, 128), 0) + 32 * mp
    qtok = jnp.where(qlane < E, qtok, qtok + 128)
    mixed = lax.rem((dp * ROWS + qtok) * 40503, 65536).astype(jnp.float32)
    dither = 1.0 - mixed * (0.5 / 65536)
    fresh = jnp.where(qtok < count, jnp.exp(logits) * dither, 0.0)
    held = fresh.astype(jnp.bfloat16)
    gt_ref[z, y] = held[:16]
    gb_ref[y, z] = held[16:]

    for k in FAR:
        send(gt_ref.at[z, y], gt_ref.at[z, y], send_sem.at[2], g_sem.at[0], (y_peer(k), mp))
        send(gb_ref.at[y, z], gb_ref.at[y, z], send_sem.at[3], g_sem.at[1], (z_peer(k), mp))

    ones = jnp.where(same, 1.0, 0.0).astype(jnp.bfloat16)
    fh, fl = split2(fresh)
    rows = f32dot(jnp.concatenate([fh, fl], axis=1), jnp.concatenate([ones, ones], axis=0))
    there = rows > 0.0
    acc = jnp.sum(fresh / jnp.where(there, rows, 1.0), axis=0, keepdims=True)
    seen = jnp.sum(jnp.where(there, 1.0, 0.0), axis=0, keepdims=True)
    both = jnp.concatenate([acc, seen], axis=0)
    ysum_ref[y] = both + pltpu.roll(both, E, 1)
    for k in FAR:
        send(ysum_ref.at[y], ysum_ref.at[y], send_sem.at[9], c_sem.at[0], (y_peer(k), mp))
    for k in (2, 1, 3):
        send(full_ref.at[mp], full_ref.at[mp], send_sem.at[1], ag_sem, (dp, x_of(k)))

    def dispatch(t):
        pz = lax.rem(z + t[0], LINE)
        py = lax.rem(y + t[1], LINE)
        peer = pz * LINE + py
        device = (peer * 2 + core, mp)
        send(comb_ref.at[:, peer], land_ref.at[spot], send_sem.at[7], d_sem, device)

    settle(comb_ref.at[0], m_sem)
    pl.semaphore_wait(known_sem, LINE - 1)
    for t in ORDER[:AHEAD]:
        dispatch(t)

    eid = eid_ref[...].astype(jnp.float32)
    eid_lo = jnp.broadcast_to(eid[:, :128], (128, 128)).T
    eid_hi = jnp.broadcast_to(eid[:, 128:], (128, 128)).T
    chosen = jnp.where(low, eid_lo, eid_hi) == lax.rem(lane, E).astype(jnp.float32)
    chosen = chosen & (jnp.where(low, row, row + 128) < count)
    mask_ref[...] = jnp.where(chosen, 1.0, 0.0)

    settle(gb_ref.at[0, pl.ds(0, LINE - 1)], g_sem.at[1])
    for k in FAR:
        send(gb_ref.at[y], gb_ref.at[y], send_sem.at[5], g_sem.at[3], (y_peer(k), mp))
    settle(ysum_ref.at[pl.ds(0, LINE - 1)], c_sem.at[0])
    zsum_ref[z] = jnp.sum(ysum_ref[...], axis=0)
    for k in FAR:
        send(zsum_ref.at[z], zsum_ref.at[z], send_sem.at[9], c_sem.at[1], (z_peer(k), mp))
    settle(gt_ref.at[0, pl.ds(0, LINE - 1)], g_sem.at[0])
    for k in FAR:
        send(gt_ref.at[z], gt_ref.at[z], send_sem.at[4], g_sem.at[2], (z_peer(k), mp))

    for s in range(2):
        land_ref[spot, s] = comb_ref[s, spot]
    me = mp * 2 + core

    def share(slots, value, rsem):
        slots[me] = value
        for k in (2, 1, 3, 0):
            for other in (1, 0):
                if k == 0 and other == 0:
                    continue
                device = (mate if other else dp, x_of(k))
                send(slots.at[me], slots.at[me], send_sem.at[8], rsem, device)

    settle(zsum_ref.at[pl.ds(0, LINE - 1)], c_sem.at[1])
    share(xsum_ref, jnp.sum(zsum_ref[...], axis=0), c_sem.at[2])

    settle(xsum_ref.at[pl.ds(0, 7)], c_sem.at[2])
    summed = jnp.sum(xsum_ref[...], axis=0)
    total = summed[1:2] * (1.0 / E)
    col = jnp.broadcast_to(total / summed[0:1], (128, 128)).T[:E]

    settle(gb_ref.at[pl.ds(0, LINE - 1)], g_sem.at[3])
    for b in range(LINE):
        aff_ref[LINE + b] = gb_ref[b].reshape(128, 128).astype(jnp.float32).T
    settle(gt_ref.at[pl.ds(0, LINE - 1)], g_sem.at[2])
    for b in range(LINE):
        aff_ref[b] = gt_ref[b].reshape(128, 128).astype(jnp.float32).T

    tile_lane = lax.broadcasted_iota(jnp.int32, (8, 128), 1)
    for it in range(ITERS - 1):
        acc = jnp.zeros((E, 128), jnp.float32)
        for b in range(2 * LINE):
            for half in range(2):
                aff = aff_ref[b, half * E : half * E + E]
                rows = jnp.sum(aff * col, axis=0, keepdims=True)
                acc = acc + aff * (1.0 / jnp.maximum(rows, TINY))
        acc = jnp.sum(acc, axis=1, keepdims=True)
        tile = jnp.ones((8, 128), jnp.float32)
        for k in range(8):
            tile = jnp.where(tile_lane == k, acc[8 * k : 8 * k + 8], tile)
        share(ar_ref.at[it], tile, ar_sem.at[it])
        if it == 0:
            for t in ORDER[AHEAD:]:
                dispatch(t)
        if it == ITERS - 2:
            before_ref[...] = jnp.concatenate([col, col], axis=0).T[0:1]
            settle(land_ref.at[pl.ds(0, SPOTS - 1)], d_sem)
            expand(land_ref, out_ref)
        settle(ar_ref.at[it, pl.ds(0, 7)], ar_sem.at[it])
        tile = total / jnp.sum(ar_ref[it], axis=0)
        if it < ITERS - 2:
            col = spread(tile)
        else:
            last_ref[...] = tile

    settle(full_ref.at[pl.ds(0, XN - 1)], ag_sem)

    settle(rs_ref, send_sem.at[0])
    settle(rs_ref, send_sem.at[1])
    settle(gt_ref.at[0, pl.ds(0, LINE - 1)], send_sem.at[2])
    settle(gt_ref.at[0, pl.ds(0, LINE - 1)], send_sem.at[3])
    settle(gt_ref.at[pl.ds(0, LINE - 1)], send_sem.at[4])
    settle(gt_ref.at[pl.ds(0, LINE - 1)], send_sem.at[5])
    settle(comb_ref.at[0], send_sem.at[6])
    settle(land_ref.at[pl.ds(0, SPOTS - 1)], send_sem.at[7])
    for _ in range(2):
        settle(ysum_ref.at[pl.ds(0, LINE - 1)], send_sem.at[9])
    settle(xsum_ref.at[pl.ds(0, 7)], send_sem.at[8])
    for it in range(ITERS - 1):
        settle(ar_ref.at[it, pl.ds(0, 7)], send_sem.at[8])


def expand(land_ref, out_ref):
    rows = 2 * GROUPS
    code = land_ref[:, :, :, WIDE:].reshape(rows, META).astype(jnp.float32).T.astype(jnp.int32)
    r = lax.broadcasted_iota(jnp.int32, (GROUPS, rows), 0)
    c = lax.broadcasted_iota(jnp.int32, (GROUPS, rows), 1)
    mine = lax.div(c, 2) == r
    second = lax.rem(c, 2)
    bits = [lax.rem(lax.div(code, 2**s), 2) for s in range(HELD)]
    below = [jnp.zeros_like(code), bits[0], bits[0] + bits[1]]
    take = [
        jnp.where(mine & (bits[s] == 1) & (below[s] == second), 1.0, 0.0) for s in range(HELD)
    ]
    take = jnp.concatenate(take, axis=0).astype(jnp.bfloat16)
    for j in range(0, WIDE, 256):
        part = land_ref[:, :, :, j : j + 256].reshape(rows, 256)
        out = f32dot(take, part).astype(jnp.bfloat16)
        out_ref[:, :, j : j + 256] = out.reshape(HELD, GROUPS, 256)


def finish(disp_ref, full_ref, mask_ref, before_ref, last_ref, out_hbm, gates_hbm, gates_ref, sem):
    put = pltpu.make_async_copy(disp_ref, out_hbm, sem.at[0])
    put.start()
    lane = lax.broadcasted_iota(jnp.int32, (128, 128), 1)
    row = lax.broadcasted_iota(jnp.int32, (128, 128), 0)
    aff = jnp.exp(full_ref[...].reshape(128, 128))
    ones = jnp.where((lane < E) == (row < E), 1.0, 0.0).astype(jnp.bfloat16)
    bh, bl = split2(aff * before_ref[...])
    rows = f32dot(bh, ones) + f32dot(bl, ones)
    last = spread(last_ref[...])
    last = jnp.concatenate([last, last], axis=0).T[0:1]
    gate = jnp.where(mask_ref[...] > 0.0, aff * last * (E / rows), 0.0)
    srow = lax.broadcasted_iota(jnp.int32, (8, 128), 0)
    slane = lax.broadcasted_iota(jnp.int32, (8, 128), 1)
    side = jnp.where(lax.div(slane, E) == srow, 1.0, 0.0).astype(jnp.bfloat16)
    g1 = gate.astype(jnp.bfloat16)
    g2, g3 = split2(gate - g1.astype(jnp.float32))
    out = ntdot(side, g1) + ntdot(side, g2) + ntdot(side, g3)
    gates_ref[...] = out[:2]
    gput = pltpu.make_async_copy(gates_ref, gates_hbm, sem.at[1])
    gput.start()
    put.wait()
    gput.wait()


def local(tokens, router_weight, valid_count, expert_id, slot_id):
    vmem = pl.BlockSpec(memory_space=pltpu.VMEM)
    hbm = pl.BlockSpec(memory_space=pltpu.HBM)
    bf, f32 = jnp.bfloat16, jnp.float32
    dma = pltpu.SemaphoreType.DMA
    parts = pl.pallas_call(
        route,
        out_shape=(
            jax.ShapeDtypeStruct((HELD, GROUPS, WIDE), bf),
            jax.ShapeDtypeStruct((XN, 32, 128), f32),
            jax.ShapeDtypeStruct((128, 128), f32),
            jax.ShapeDtypeStruct((1, 128), f32),
            jax.ShapeDtypeStruct((8, 128), f32),
        ),
        in_specs=[pl.BlockSpec(memory_space=pltpu.SMEM), *[hbm] * 4],
        out_specs=(vmem,) * 5,
        scratch_shapes=[
            pltpu.VMEM((1, ROWS), jnp.int32),
            pltpu.VMEM((1, ROWS), jnp.int32),
            pltpu.VMEM((E, WIDE), bf),
            pltpu.VMEM((ROWS, WIDE), bf),
            pltpu.VMEM((2, SPOTS, 2, WIDE + META), bf),
            pltpu.VMEM((2, SPOTS, 2, WIDE + META), bf),
            pltpu.VMEM((SPOTS, 2, 2, WIDE + META), bf),
            pltpu.VMEM((XN, 32, 128), f32),
            pltpu.VMEM((XN - 1, 32, 128), f32),
            pltpu.VMEM((LINE, LINE, 16, 128), bf),
            pltpu.VMEM((LINE, LINE, 16, 128), bf),
            pltpu.VMEM((8, 2, 128), f32),
            pltpu.VMEM((ITERS - 1, 8, 8, 128), f32),
            pltpu.VMEM((LINE, 2, 128), f32),
            pltpu.VMEM((LINE, 2, 128), f32),
            pltpu.VMEM((2 * LINE, 128, 128), f32),
            dma((4,)), dma((10,)), dma, dma, dma((4,)), dma((ITERS - 1,)), dma, dma, dma((3,)),
            pltpu.SemaphoreType.REGULAR,
        ],
        compiler_params=pltpu.CompilerParams(
            collective_id=0, has_side_effects=True, vmem_limit_bytes=24 * 2**20
        ),
        name="route",
    )(valid_count, *(
        pltpu.with_memory_space_constraint(x, pltpu.HBM)
        for x in (
            expert_id.reshape(1, ROWS), slot_id.reshape(1, ROWS),
            router_weight.T, tokens,
        )
    ))
    dispatched, gates = pl.pallas_call(
        finish,
        out_shape=(
            jax.ShapeDtypeStruct((HELD, GROUPS, WIDE), bf),
            jax.ShapeDtypeStruct((2, 128), f32),
        ),
        in_specs=[vmem] * 5,
        out_specs=(hbm, hbm),
        scratch_shapes=[pltpu.VMEM((2, 128), f32), dma((2,))],
        compiler_params=pltpu.CompilerParams(vmem_limit_bytes=16 * 2**20),
        name="finish",
    )(*parts)
    return gates.reshape(ROWS), dispatched


def solution(mesh):
    return jax.shard_map(
        local,
        mesh=mesh,
        in_specs=(P("dp", "mp"), P("mp", None), P("dp"), P("dp"), P("dp")),
        out_specs=(P("dp"), P("dp", None, "mp")),
        check_vma=False,
    )
```
